32 devices in a mesh: expert: 16 (over z, y, core), dp: 2 (over x).
Axes of the slice: x: 2, y: 2, z: 4, core: 2. Of those that a mesh axis runs over, the one named last changes fastest.
Arguments:
- tokens: bfloat16 [4096, 4096], P(('expert', 'dp')), may hold values from -6 to 6
- route: int32 [4096, 2], P(('expert', 'dp')), may hold values from 0 to 31, all different within a row; in each aligned block of 128 rows (0 to 127, 128 to 255, ...) at most 24 rows name the same one
- gate_output_gradient: bfloat16 [4096, 2, 1536], P(('expert', 'dp')), may hold values from -0.4375 to 0.4375
- frozen_gate_weight: bfloat16 [32, 4096, 1536], P('expert', 'dp'), may hold values from -0.09375 to 0.09375
- adapter_first: bfloat16 [32, 4096, 16], P('expert'), may hold values from -0.09375 to 0.09375
- adapter_second: bfloat16 [32, 16, 1536], P('expert'), may hold values from -0.15625 to 0.15625
Outputs:
- grad_a: float32 [32, 4096, 16], P('expert')
- grad_b: float32 [32, 16, 1536], P('expert')
The draws below stay inside these ranges and needn't reach their ends.
Inputs may be any that keep to these rules, and one draw needn't show every extreme that they name: `route`: each row names 2 different experts. Within each device's aligned block of 128 rows no expert is named more than 24 times.
All inputs are finite; a program needn't handle non-finite values.
Results may differ from the reference program's by a relative error of at most 0.0043.
Values may be sent and summed in bfloat16 or wider, within the bound.
A program may use at most 128 MiB of HBM per device.

```python
import math
import jax
import jax.numpy as jnp
import numpy as np
from jax import lax

MODEL_WIDTH = 4096
GATE_HIDDEN = 1536
ADAPTER_RANK = 16
TOP = 2
TOK_DEV = 128
EXPERT_TOTAL = 32
CAP = 24
TOKENS = 4096


def levels(own_key, shape, pieces, low, high):
    gain, own = 1.0, jax.random.fold_in(own_key, 6)
    for dim, parts in pieces:
        heights = jnp.exp(jax.random.uniform(jax.random.fold_in(own, dim), (parts,), jnp.float32, low / len(pieces), high / len(pieces)))
        gain = gain * jnp.repeat(heights, shape[dim] // parts).reshape([-1 if axis == dim else 1 for axis in range(len(shape))])
    return gain


def assign_block(stream_key, own, number, rows, amount, top, bound, lean):
    order = jax.random.permutation(stream_key, amount)
    heavy_load, common = load_shares(amount, rows * top, bound, lean, True), load_shares(amount, rows * top, bound, lean, False)
    places = jnp.arange(amount)

    def named(sizes, rotation):
        used = int((sizes > 0).sum())
        fixed = max(1, used // 4)
        shifted = fixed + (places - fixed + rotation * (used - fixed)) % max(1, amount - fixed)
        return jnp.zeros((amount,), jnp.int32).at[order[jnp.where(places < fixed, places, shifted)]].set(jnp.asarray(sizes, jnp.int32))

    sizes = jnp.where(number % 4 == 0, named(heavy_load, number // 4), named(common, number - number // 4 - 1))
    mixed = jax.random.permutation(jax.random.fold_in(own, 3), amount)
    source_of, receiver = mixed[0:amount // 2 * 2:2], mixed[1:amount // 2 * 2:2]
    slack = jnp.minimum(sizes[source_of] - 1, bound - sizes[receiver]) // 2
    slack = jnp.where((source_of == order[0]) | (receiver == order[0]) | (sizes[receiver] == 0), 0, jnp.maximum(slack, 0))
    shifted = jax.random.randint(jax.random.fold_in(own, 4), (amount // 2,), 0, 1 << 20) % (slack + 1)
    sizes = sizes.at[source_of].add(-shifted).at[receiver].add(shifted)
    items = jnp.searchsorted(jnp.cumsum(sizes), jnp.arange(rows * top), side="right").astype(jnp.int32)
    table = items.reshape(top, rows).T
    table = table[jax.random.permutation(jax.random.fold_in(own, 1), rows)]
    rotation = jax.random.randint(jax.random.fold_in(own, 2), (rows, 1), 0, top)
    return jnp.take_along_axis(table, (jnp.arange(top)[None, :] + rotation) % top, axis=1)


def load_shares(amount, total, limit, lean, full):
    portions = [(1 << 20) // math.isqrt(standing ** lean) + 1 for standing in range(1, amount + 1)]
    largest = limit if full else min(limit, max(-(-total // amount), total * portions[0] // sum(portions)))
    least = 1 if total - largest >= amount - 1 else 0
    given, rest = [largest] + [least] * (amount - 1), total - largest - least * (amount - 1)
    while rest > 0:
        movable = [i for i in range(1, amount) if given[i] < largest] or [i for i in range(1, amount) if given[i] < limit]
        pool, budget = sum([portions[i] for i in movable]), rest
        for i in movable:
            extra = min(limit - given[i], max(1, budget * portions[i] // pool), rest)
            given[i] = given[i] + extra
            rest = rest - extra
    return np.array(given)


def gaussian(rng, shape, deviation, most, split=(), kind=jnp.bfloat16):
    gain = levels(rng, shape, split, -0.22, 0.18) if split else 1.0
    drawn = jax.random.normal(rng, shape, jnp.float32) * deviation * gain
    return jnp.minimum(jnp.maximum(drawn, -most), most).astype(kind)


def setup_inputs(seed: int = 0) -> dict:
    splits = jax.random.split(jax.random.key(seed), 7)
    tokens = gaussian(splits[0], (TOKENS, MODEL_WIDTH), 1.0, 6.0, ((0, 32),))
    route_keys = jax.random.split(jax.random.fold_in(splits[1], 1), TOKENS // TOK_DEV)
    route_turns = jax.random.permutation(jax.random.fold_in(splits[1], 3), TOKENS // TOK_DEV)
    route = jax.vmap(lambda own, number: assign_block(jax.random.fold_in(splits[1], 2), own, number, TOK_DEV, EXPERT_TOTAL, TOP, CAP, 2))(route_keys, route_turns).reshape((TOKENS, TOP))
    gate_output_gradient = gaussian(splits[2], (TOKENS, TOP, GATE_HIDDEN), 0.03, 0.4375, ((0, 32),))
    frozen_gate_weight = gaussian(splits[3], (EXPERT_TOTAL, MODEL_WIDTH, GATE_HIDDEN), MODEL_WIDTH ** -0.5, 0.09375, ((0, 16), (1, 2)))
    adapter_first = gaussian(splits[4], (EXPERT_TOTAL, MODEL_WIDTH, ADAPTER_RANK), MODEL_WIDTH ** -0.5, 0.09375, ((0, 16),))
    adapter_second = gaussian(splits[5], (EXPERT_TOTAL, ADAPTER_RANK, GATE_HIDDEN), GATE_HIDDEN ** -0.5, 0.15625, ((0, 16),))
    return dict(tokens=tokens, route=route, gate_output_gradient=gate_output_gradient, frozen_gate_weight=frozen_gate_weight, adapter_first=adapter_first, adapter_second=adapter_second)


ADAPTER_SCALE = 2.0


def silu_slope(gate_preactivation):
    squash = jax.nn.sigmoid(gate_preactivation)
    return squash * (1.0 + gate_preactivation * (1.0 - squash))


def reference(tokens, route, gate_output_gradient, frozen_gate_weight, adapter_first, adapter_second):
    group_rows = 512
    slot_count = TOKENS * TOP
    flat_route = route.reshape(slot_count).astype(jnp.int32)
    order = jnp.argsort(flat_route, stable=True).astype(jnp.int32)
    labels = jnp.arange(EXPERT_TOTAL, dtype=jnp.int32)
    counts = jnp.sum((flat_route[:, None] == labels[None, :]).astype(jnp.int32), axis=0)
    starts = jnp.cumsum(counts) - counts
    padded = (counts + group_rows - 1) // group_rows * group_rows
    pad_starts = jnp.cumsum(padded) - padded
    block_count = slot_count // group_rows + EXPERT_TOTAL
    flat_grad = gate_output_gradient.reshape(slot_count, GATE_HIDDEN)

    def one_block(carry, block_index):
        down_gradient, up_gradient = carry
        first = block_index * group_rows
        expert_index = (jnp.sum((pad_starts <= first).astype(jnp.int32)) - 1).astype(jnp.int32)
        within = first + jnp.arange(group_rows, dtype=jnp.int32) - pad_starts[expert_index]
        valid = within < counts[expert_index]
        source = order[jnp.clip(starts[expert_index] + within, 0, slot_count - 1)]
        input_rows = tokens[source // TOP]
        rows_g = jnp.where(valid[:, None], flat_grad[source], jnp.zeros((), flat_grad.dtype))
        weight = frozen_gate_weight[expert_index]
        first_adapter_factor = adapter_first[expert_index]
        second_adapter_factor = adapter_second[expert_index]
        frozen_output = jnp.dot(input_rows, weight, preferred_element_type=jnp.float32)
        rank_reduced_output = jnp.dot(input_rows, first_adapter_factor, preferred_element_type=jnp.float32).astype(jnp.bfloat16)
        gate_preactivation = frozen_output + ADAPTER_SCALE * jnp.dot(rank_reduced_output, second_adapter_factor, preferred_element_type=jnp.float32)
        activation_slope = (rows_g.astype(jnp.float32) * silu_slope(gate_preactivation)).astype(jnp.bfloat16)
        up_portion = ADAPTER_SCALE * jnp.dot(rank_reduced_output.T, activation_slope, preferred_element_type=jnp.float32)
        rank_backward = jnp.dot(activation_slope, second_adapter_factor.T, preferred_element_type=jnp.float32).astype(jnp.bfloat16)
        down_portion = ADAPTER_SCALE * jnp.dot(input_rows.T, rank_backward, preferred_element_type=jnp.float32)
        down_gradient = down_gradient.at[expert_index].add(down_portion)
        up_gradient = up_gradient.at[expert_index].add(up_portion)
        return (down_gradient, up_gradient), None

    initial = (jnp.zeros((EXPERT_TOTAL, MODEL_WIDTH, ADAPTER_RANK), jnp.float32), jnp.zeros((EXPERT_TOTAL, ADAPTER_RANK, GATE_HIDDEN), jnp.float32))
    (grad_a, grad_b), _ = lax.scan(one_block, initial, jnp.arange(block_count, dtype=jnp.int32))
    return grad_a, grad_b
```

```python
import functools

import jax
import jax.numpy as jnp
from jax import lax
from jax.experimental import pallas as pl
from jax.experimental.pallas import tpu as pltpu
from jax.sharding import PartitionSpec as P

ADAPTER_SCALE = 2.0
RING = 4
F32 = jnp.float32


def silu_slope(gate_preactivation):
    squash = jax.nn.sigmoid(gate_preactivation)
    return squash * (1.0 + gate_preactivation * (1.0 - squash))


def dot(spec, a, b):
    return jnp.einsum(spec, a, b, preferred_element_type=F32)


def slot_codes(route, experts, capacity):
    tok_rows, top_count = route.shape
    flat_route = route.reshape(tok_rows * top_count)
    labels = jnp.arange(experts, dtype=jnp.int32)
    one_hot = (flat_route[:, None] == labels[None, :]).astype(jnp.int32)
    ranks = jnp.sum((jnp.cumsum(one_hot, axis=0) - one_hot) * one_hot, axis=1)
    return (flat_route * capacity + ranks).reshape(tok_rows, top_count)


def spread_kernel(columns, halves, own_ref, all_ref, send_sems, recv_sems):
    column, me = lax.axis_index("expert"), lax.axis_index("dp")
    total = columns * halves
    here = column * halves + me

    def peer(k):
        there = lax.rem(here + k, total)
        return (lax.div(there, halves), lax.rem(there, halves))

    barrier = pltpu.get_barrier_semaphore()

    @pl.loop(1, total)
    def _(k):
        pl.semaphore_signal(
            barrier, inc=1, device_id=peer(k), device_id_type=pl.DeviceIdType.MESH
        )

    pl.semaphore_wait(barrier, total - 1)

    def copy(k, slot):
        return pltpu.make_async_remote_copy(
            src_ref=own_ref,
            dst_ref=all_ref.at[slot],
            send_sem=send_sems.at[k],
            recv_sem=recv_sems.at[k],
            device_id=peer(k),
            device_id_type=pl.DeviceIdType.MESH,
        )

    @pl.loop(1, total)
    def _(k):
        copy(k, here).start()

    all_ref[here] = own_ref[...]

    @pl.loop(1, total)
    def _(k):
        copy(k, lax.rem(here + total - k, total)).wait()


def spread(value, columns, halves):
    total = columns * halves
    return pl.pallas_call(
        functools.partial(spread_kernel, columns, halves),
        out_shape=jax.ShapeDtypeStruct((total, *value.shape), value.dtype),
        in_specs=[pl.BlockSpec(memory_space=pltpu.VMEM)],
        out_specs=pl.BlockSpec(memory_space=pltpu.VMEM),
        scratch_shapes=[
            pltpu.SemaphoreType.DMA((total,)),
            pltpu.SemaphoreType.DMA((total,)),
        ],
        compiler_params=pltpu.CompilerParams(collective_id=0, has_side_effects=True),
        name="spread",
    )(value)


def local(tokens, route, gate_output_gradient, frozen_gate_weight, adapter_first, adapter_second):
    experts_here, part, hidden = frozen_gate_weight.shape
    columns, halves = lax.axis_size("expert"), lax.axis_size("dp")
    experts = experts_here * columns
    tok_rows, width = tokens.shape
    top_count = route.shape[1]
    capacity = 3 * tok_rows * top_count // experts
    hidden_part = hidden // halves
    ring = RING if columns % RING == 0 else 1
    inner = columns // ring
    column, me = lax.axis_index("expert"), lax.axis_index("dp")
    outer_at, inner_at = column // inner, column % inner

    codes = slot_codes(route, experts, capacity)
    all_codes = spread(codes.T, columns, halves).transpose(0, 2, 1).reshape(
        columns, halves, tok_rows, top_count
    )

    def piece(target):
        parts = [lax.dynamic_slice_in_dim(tokens, target * part, part, 1)]
        for k in range(top_count):
            parts.append(
                lax.dynamic_slice_in_dim(
                    gate_output_gradient[:, k], target * hidden_part, hidden_part, 1
                )
            )
        return jnp.concatenate(parts, axis=1)

    def dp_shift(value, k):
        return lax.ppermute(value, "dp", [(i, (i + k) % halves) for i in range(halves)])

    def dp_sum(value):
        total = value
        for k in range(1, halves):
            total = total + dp_shift(jnp.roll(value, k, axis=1), k)
        return total

    streams = [(piece(me)[None], [0])]
    if halves > 1:
        others = [dp_shift(piece((me + k) % halves), k) for k in range(1, halves)]
        streams.append((jnp.stack(others), list(range(1, halves))))

    around = [(i, (i + inner) % columns) for i in range(columns)]
    first_part = lax.dynamic_slice_in_dim(adapter_first, me * part, part, 1)
    second_part = lax.dynamic_slice_in_dim(adapter_second, me * hidden_part, hidden_part, 2)
    group = experts_here * capacity
    places = (
        (outer_at * inner + (inner_at + jnp.arange(inner, dtype=jnp.int32)) % inner)[:, None]
        * group
        + jnp.arange(group, dtype=jnp.int32)[None, :]
    ).reshape(inner * group)

    grad_a, grad_b = 0.0, 0.0
    blocks = [stream[0] for stream in streams]
    for step in range(ring):
        source = (outer_at + ring - step) % ring * inner + inner_at
        step_codes = lax.dynamic_index_in_dim(all_codes, source, 0, keepdims=False)
        following, step_rows = [], []
        for (_, shifts), block in zip(streams, blocks):
            if step < ring - 1:
                following.append(lax.ppermute(block, "expert", around))
            count = len(shifts)
            own_codes = jnp.stack(
                [
                    lax.dynamic_index_in_dim(step_codes, (me + halves - k) % halves, 0, keepdims=False)
                    for k in shifts
                ]
            )
            picks = [
                (own_codes[:, None, :, k] == places[None, :, None]).astype(jnp.bfloat16)
                for k in range(top_count)
            ]
            packed_x = dot("mrt,mtw->mrw", sum(picks[1:], picks[0]), block[:, :, :part])
            packed_g = sum(
                dot(
                    "mrt,mtw->mrw",
                    picks[k],
                    block[:, :, part + k * hidden_part : part + (k + 1) * hidden_part],
                )
                for k in range(top_count)
            )
            packed = jnp.concatenate(
                [packed_x.astype(jnp.bfloat16), packed_g.astype(jnp.bfloat16)], axis=2
            ).reshape(count, inner, group, part + hidden_part)
            arrived = [packed[:, 0]]
            for j in range(1, inner):
                pairs = [
                    (o * inner + i, o * inner + (i + j) % inner)
                    for o in range(ring)
                    for i in range(inner)
                ]
                arrived.append(lax.ppermute(packed[:, j], "expert", pairs))
            step_rows.append(
                jnp.stack(arrived, 1).reshape(count, inner, experts_here, capacity, -1)
            )
        rows = jnp.concatenate(step_rows, axis=0).transpose(2, 0, 1, 3, 4)
        rows = rows.reshape(experts_here, halves, inner * capacity, -1)
        rows_x, rows_g = rows[..., :part], rows[..., part:]
        partial = dot("ednw,ewf->ednf", rows_x, frozen_gate_weight)
        low = dp_sum(dot("ednw,ewr->ednr", rows_x, first_part)).astype(jnp.bfloat16)

        def take(target):
            return lax.dynamic_slice_in_dim(partial, target * hidden_part, hidden_part, 3)

        preact = take(me) + ADAPTER_SCALE * dot("ednr,erf->ednf", low, second_part)
        for k in range(1, halves):
            sent = jnp.roll(take((me + k) % halves).astype(jnp.bfloat16), k, axis=1)
            preact = preact + dp_shift(sent, k).astype(F32)
        slope = (rows_g.astype(F32) * silu_slope(preact)).astype(jnp.bfloat16)
        back = dp_sum(dot("ednf,erf->ednr", slope, second_part)).astype(jnp.bfloat16)
        grad_b = grad_b + dot("ednr,ednf->erf", low, slope)
        grad_a = grad_a + dot("ednr,ednw->erw", back, rows_x)
        blocks = following

    joined = ADAPTER_SCALE * jnp.concatenate([grad_a, grad_b], axis=2)
    pieces = [joined] + [dp_shift(joined, k) for k in range(1, halves)]
    stacked = jnp.stack(pieces[::-1])
    whole = jnp.roll(stacked, me + 1, axis=0)
    whole_a = whole[:, :, :, :part].transpose(1, 0, 3, 2).reshape(experts_here, width, -1)
    whole_b = whole[:, :, :, part:].transpose(1, 2, 0, 3).reshape(experts_here, -1, hidden)
    return (whole_a, whole_b)


def solution(mesh):
    return jax.shard_map(
        local,
        mesh=mesh,
        in_specs=(
            P(("expert", "dp"), None),
            P(("expert", "dp"), None),
            P(("expert", "dp"), None, None),
            P("expert", "dp", None),
            P("expert", None, None),
            P("expert", None, None),
        ),
        out_specs=(P("expert", None, None), P("expert", None, None)),
        check_vma=False,
    )
```

```python
import functools

import jax
import jax.numpy as jnp
from jax import lax
from jax.experimental import pallas as pl
from jax.experimental.pallas import tpu as pltpu
from jax.sharding import PartitionSpec as P

ADAPTER_SCALE = 2.0
RING = 4
F32 = jnp.float32


def silu_slope(gate_preactivation):
    squash = jax.nn.sigmoid(gate_preactivation)
    return squash * (1.0 + gate_preactivation * (1.0 - squash))


def dot(spec, a, b):
    return jnp.einsum(spec, a, b, preferred_element_type=F32)


def slot_codes(route, experts, capacity):
    tok_rows, top_count = route.shape
    flat_route = route.reshape(tok_rows * top_count)
    labels = jnp.arange(experts, dtype=jnp.int32)
    one_hot = (flat_route[:, None] == labels[None, :]).astype(jnp.int32)
    ranks = jnp.sum((jnp.cumsum(one_hot, axis=0) - one_hot) * one_hot, axis=1)
    return (flat_route * capacity + ranks).reshape(tok_rows, top_count)


def spread_kernel(columns, halves, own_ref, all_ref, send_sems, recv_sems):
    column, me = lax.axis_index("expert"), lax.axis_index("dp")
    total = columns * halves
    here = column * halves + me

    def peer(k):
        there = lax.rem(here + k, total)
        return (lax.div(there, halves), lax.rem(there, halves))

    barrier = pltpu.get_barrier_semaphore()

    @pl.loop(1, total)
    def _(k):
        pl.semaphore_signal(
            barrier, inc=1, device_id=peer(k), device_id_type=pl.DeviceIdType.MESH
        )

    pl.semaphore_wait(barrier, total - 1)

    def copy(k, slot):
        return pltpu.make_async_remote_copy(
            src_ref=own_ref,
            dst_ref=all_ref.at[slot],
            send_sem=send_sems.at[k],
            recv_sem=recv_sems.at[k],
            device_id=peer(k),
            device_id_type=pl.DeviceIdType.MESH,
        )

    @pl.loop(1, total)
    def _(k):
        copy(k, here).start()

    all_ref[here] = own_ref[...]

    @pl.loop(1, total)
    def _(k):
        copy(k, lax.rem(here + total - k, total)).wait()


def spread(value, columns, halves):
    total = columns * halves
    return pl.pallas_call(
        functools.partial(spread_kernel, columns, halves),
        out_shape=jax.ShapeDtypeStruct((total, *value.shape), value.dtype),
        in_specs=[pl.BlockSpec(memory_space=pltpu.VMEM)],
        out_specs=pl.BlockSpec(memory_space=pltpu.VMEM),
        scratch_shapes=[
            pltpu.SemaphoreType.DMA((total,)),
            pltpu.SemaphoreType.DMA((total,)),
        ],
        compiler_params=pltpu.CompilerParams(collective_id=0, has_side_effects=True),
        name="spread",
    )(value)


def local(tokens, route, gate_output_gradient, frozen_gate_weight, adapter_first, adapter_second):
    experts_here, part, hidden = frozen_gate_weight.shape
    columns, halves = lax.axis_size("expert"), lax.axis_size("dp")
    experts = experts_here * columns
    tok_rows, width = tokens.shape
    top_count = route.shape[1]
    capacity = 3 * tok_rows * top_count // experts
    hidden_part = hidden // halves
    ring = RING if columns % RING == 0 else 1
    inner = columns // ring
    column, me = lax.axis_index("expert"), lax.axis_index("dp")
    outer_at, inner_at = column // inner, column % inner

    codes = slot_codes(route, experts, capacity)
    all_codes = spread(codes.T, columns, halves).transpose(0, 2, 1).reshape(
        columns, halves, tok_rows, top_count
    )

    def piece(target):
        parts = [lax.dynamic_slice_in_dim(tokens, target * part, part, 1)]
        for k in range(top_count):
            parts.append(
                lax.dynamic_slice_in_dim(
                    gate_output_gradient[:, k], target * hidden_part, hidden_part, 1
                )
            )
        return jnp.concatenate(parts, axis=1)

    def dp_shift(value, k):
        return lax.ppermute(value, "dp", [(i, (i + k) % halves) for i in range(halves)])

    def dp_sum(value):
        total = value
        for k in range(1, halves):
            total = total + dp_shift(jnp.roll(value, k, axis=1), k)
        return total

    streams = [(piece(me)[None], [0])]
    if halves > 1:
        others = [dp_shift(piece((me + k) % halves), k) for k in range(1, halves)]
        streams.append((jnp.stack(others), list(range(1, halves))))

    around = [(i, (i + inner) % columns) for i in range(columns)]
    first_part = lax.dynamic_slice_in_dim(adapter_first, me * part, part, 1)
    second_part = lax.dynamic_slice_in_dim(adapter_second, me * hidden_part, hidden_part, 2)
    group = experts_here * capacity
    places = (
        (outer_at * inner + (inner_at + jnp.arange(inner, dtype=jnp.int32)) % inner)[:, None]
        * group
        + jnp.arange(group, dtype=jnp.int32)[None, :]
    ).reshape(inner * group)

    grad_a, grad_b = 0.0, 0.0
    blocks = [stream[0] for stream in streams]
    for step in range(ring):
        source = (outer_at + ring - step) % ring * inner + inner_at
        step_codes = lax.dynamic_index_in_dim(all_codes, source, 0, keepdims=False)
        following, step_rows = [], []
        for (_, shifts), block in zip(streams, blocks):
            if step < ring - 1:
                following.append(lax.ppermute(block, "expert", around))
            count = len(shifts)
            own_codes = jnp.stack(
                [
                    lax.dynamic_index_in_dim(step_codes, (me + halves - k) % halves, 0, keepdims=False)
                    for k in shifts
                ]
            )
            picks = [
                (own_codes[:, None, :, k] == places[None, :, None]).astype(jnp.bfloat16)
                for k in range(top_count)
            ]
            packed_x = dot("mrt,mtw->mrw", sum(picks[1:], picks[0]), block[:, :, :part])
            packed_g = sum(
                dot(
                    "mrt,mtw->mrw",
                    picks[k],
                    block[:, :, part + k * hidden_part : part + (k + 1) * hidden_part],
                )
                for k in range(top_count)
            )
            packed = jnp.concatenate(
                [packed_x.astype(jnp.bfloat16), packed_g.astype(jnp.bfloat16)], axis=2
            ).reshape(count, inner, group, part + hidden_part)
            arrived = [packed[:, 0]]
            for j in range(1, inner):
                pairs = [
                    (o * inner + i, o * inner + (i + j) % inner)
                    for o in range(ring)
                    for i in range(inner)
                ]
                arrived.append(lax.ppermute(packed[:, j], "expert", pairs))
            step_rows.append(
                jnp.stack(arrived, 1).reshape(count, inner, experts_here, capacity, -1)
            )
        rows = jnp.concatenate(step_rows, axis=0).transpose(2, 0, 1, 3, 4)
        rows = rows.reshape(experts_here, halves, inner * capacity, -1)
        rows_x, rows_g = rows[..., :part], rows[..., part:]
        partial = dot("ednw,ewf->ednf", rows_x, frozen_gate_weight)
        low = dp_sum(dot("ednw,ewr->ednr", rows_x, first_part)).astype(jnp.bfloat16)

        def take(target):
            return lax.dynamic_slice_in_dim(partial, target * hidden_part, hidden_part, 3)

        preact = take(me) + ADAPTER_SCALE * dot("ednr,erf->ednf", low, second_part)
        for k in range(1, halves):
            sent = jnp.roll(take((me + k) % halves).astype(jnp.bfloat16), k, axis=1)
            preact = preact + dp_shift(sent, k).astype(F32)
        slope = (rows_g.astype(F32) * silu_slope(preact)).astype(jnp.bfloat16)
        back = dp_sum(dot("ednf,erf->ednr", slope, second_part)).astype(jnp.bfloat16)
        grad_b = grad_b + dot("ednr,ednf->erf", low, slope)
        grad_a = grad_a + dot("ednr,ednw->erw", back, rows_x)
        blocks = following

    joined = ADAPTER_SCALE * jnp.concatenate([grad_a, grad_b], axis=2)
    pieces = [joined] + [dp_shift(joined, k) for k in range(1, halves)]
    stacked = jnp.stack(pieces[::-1])
    whole = jnp.roll(stacked, me + 1, axis=0)
    whole_a = whole[:, :, :, :part].transpose(1, 0, 3, 2).reshape(experts_here, width, -1)
    whole_b = whole[:, :, :, part:].transpose(1, 2, 0, 3).reshape(experts_here, -1, hidden)
    return (whole_a, whole_b)


MESH = pl.DeviceIdType.MESH
LANES = 256


def chunks(extent, size, body):
    def step(n, carry):
        body(pl.ds(pl.multiple_of(n * size, size), size))
        return carry

    lax.fori_loop(0, extent // size, step, 0)


def whole_kernel(
    ring, inner, capacity,
    tok, grd, route, wgt, first, second,
    out_a, out_b,
    blk_c, blk_x, blk_g, stg_x, stg_g, row_x, row_g, w_buf, srt, pre, slope, lowb,
    snd_p, rcv_p, snd_l, rcv_l, snd_b, rcv_b, acc_a, acc_b,
    loc_sem, dps_sem, dpr_sem, zs_sem, zr_sem, ps_sem, pr_sem, qs_sem, qr_sem, bs_sem, br_sem,
    fs_sem, fr_sem,
):
    column, me = lax.axis_index("expert"), lax.axis_index("dp")
    z, p0 = column // inner, column % inner
    other = 1 - me
    experts_here, part, hidden = w_buf.shape
    half = hidden // 2
    tok_rows = tok.shape[0]
    group = experts_here * capacity
    total_rows = inner * group
    each = inner * capacity
    experts = experts_here * inner * ring
    last = ring - 1
    inside = (z > 0) & (z < last)

    def unit(k):
        near = jnp.where(inside, jnp.where(k == 1, 2, jnp.where(k == 2, 0, k)), k)
        flipped = jnp.where(z < ring // 2, near, last - near)
        return jnp.where(k == 0, z, flipped)

    barrier = pltpu.get_barrier_semaphore()

    def greet(device):
        pl.semaphore_signal(barrier, inc=1, device_id=device, device_id_type=MESH)

    for p in range(1, inner):
        greet((z * inner + (p0 + p) % inner, me))
    greet((column, other))

    @pl.when(z > 0)
    def _():
        greet((column - inner, me))

    @pl.when(z < last)
    def _():
        greet((column + inner, me))

    pl.semaphore_wait(
        barrier, inner + jnp.where(z > 0, 1, 0) + jnp.where(z < last, 1, 0)
    )

    my_cols = pl.ds(pl.multiple_of(me * part, part), part)
    its_cols = pl.ds(pl.multiple_of(other * part, part), part)
    my_hid = pl.ds(pl.multiple_of(me * half, half), half)
    its_hid = pl.ds(pl.multiple_of(other * half, half), half)
    blocks = (blk_c, blk_x, blk_g)

    def remote(src, dst, send, recv, device):
        return pltpu.make_async_remote_copy(
            src_ref=src, dst_ref=dst, send_sem=send, recv_sem=recv,
            device_id=device, device_id_type=MESH,
        )

    local_x = pltpu.make_async_copy(tok.at[:, my_cols], blk_x.at[z, 0], loc_sem.at[0])
    local_g = pltpu.make_async_copy(grd.at[:, :, my_hid], blk_g.at[z, 0], loc_sem.at[1])
    local_w = pltpu.make_async_copy(wgt, w_buf, loc_sem.at[2])

    def dp_copy(item):
        src = (blk_c.at[z, 0], tok.at[:, its_cols], grd.at[:, :, its_hid])[item]
        return remote(
            src, blocks[item].at[z, 1], dps_sem.at[item], dpr_sem.at[item], (column, other)
        )

    def z_copy(way, u, s, item, src=None):
        step = inner if way == 0 else -inner
        dst = blocks[item].at[u, s]
        return remote(
            dst if src is None else src, dst,
            zs_sem.at[way, u, s, item], zr_sem.at[u, s, item], (column + step, me),
        )

    def z_send(u, s, item, up, down, src=None):
        @pl.when(up & (z < last))
        def _():
            z_copy(0, u, s, item, src).start()

        @pl.when(down & (z > 0))
        def _():
            z_copy(1, u, s, item, src).start()

    def relay(u, s, item):
        z_copy(0, u, s, item).wait_recv()
        z_send(u, s, item, u < z, u > z)

    yes = z >= 0
    local_x.start()
    dp_copy(1).start()
    z_send(z, 0, 1, yes, yes, tok.at[:, my_cols])
    local_g.start()
    dp_copy(2).start()

    labels = lax.broadcasted_iota(jnp.int32, (experts, tok_rows), 0)
    ones = [jnp.where(route[k : k + 1, :] == labels, 1.0, 0.0) for k in range(2)]
    earlier = jnp.where(
        lax.broadcasted_iota(jnp.int32, (tok_rows, tok_rows), 0)
        < lax.broadcasted_iota(jnp.int32, (tok_rows, tok_rows), 1),
        1.0,
        0.0,
    ).astype(jnp.bfloat16)
    before = [
        jnp.dot(one.astype(jnp.bfloat16), earlier, preferred_element_type=F32) for one in ones
    ]
    before[1] = before[1] + jnp.sum(ones[0], axis=1, keepdims=True)
    base = lax.broadcasted_iota(jnp.int32, (experts, tok_rows), 0).astype(F32) * capacity
    blk_c[z, 0] = jnp.zeros(blk_c.shape[2:], jnp.int32)
    for k in range(2):
        code = jnp.sum(ones[k] * (before[k] + base), axis=0, keepdims=True)
        blk_c[z, 0, k : k + 1, :] = code.astype(jnp.int32)
    dp_copy(0).start()
    z_send(z, 0, 0, yes, yes)
    local_w.start()

    def plane_copy(kind, u, s, p):
        stage, rows = ((stg_x, row_x), (stg_g, row_g))[kind]
        peer = (p0 + p) % inner
        return remote(
            stage.at[u, s, pl.ds(pl.multiple_of(peer * group, group), group), :],
            rows.at[u, s, pl.ds(pl.multiple_of(p0 * group, group), group), :],
            ps_sem.at[kind, u, s, p], pr_sem.at[kind, u, s, p], (z * inner + peer, me),
        )

    def plane_wait(kind, u, s):
        for p in range(1, inner):
            plane_copy(kind, u, s, p).wait_recv()

    def pack(kind, u, s):
        place = z * total_rows + lax.broadcasted_iota(
            jnp.int32, (total_rows, tok_rows), 0
        )
        picks = [blk_c[u, s, k : k + 1, :] == place for k in range(2)]
        stage, rows = ((stg_x, row_x), (stg_g, row_g))[kind]
        if kind == 0:
            chosen = jnp.where(picks[0] | picks[1], 1.0, 0.0).astype(jnp.bfloat16)
        else:
            chosen = jnp.concatenate(
                [jnp.where(pick, 1.0, 0.0).astype(jnp.bfloat16) for pick in picks], axis=1
            )

        def one(cols):
            if kind == 0:
                block = blk_x[u, s, :, cols]
            else:
                block = blk_g[u, s, :, :, cols].reshape(2 * tok_rows, LANES)
            stage[u, s, :, cols] = jnp.dot(
                chosen, block, preferred_element_type=F32
            ).astype(jnp.bfloat16)

        chunks(stage.shape[-1], LANES, one)
        mine = pl.ds(pl.multiple_of(p0 * group, group), group)
        rows[u, s, mine, :] = stage[u, s, mine, :]
        for p in range(1, inner):
            plane_copy(kind, u, s, p).start()

    def partner_copy(u, s, item):
        src, dst = ((snd_p, rcv_p), (snd_l, rcv_l))[item]
        return remote(
            src.at[u, s], dst.at[u, 1 - s], qs_sem.at[u, s, item], qr_sem.at[u, 1 - s, item],
            (column, other),
        )

    def partner_wait(u, s, item):
        src, dst = ((snd_p, rcv_p), (snd_l, rcv_l))[item]
        remote(
            src.at[u, s], dst.at[u, s], qs_sem.at[u, s, item], qr_sem.at[u, s, item],
            (column, other),
        ).wait_recv()

    def matmul(u, s):
        plane_wait(0, u, s)

        def sort(cols):
            wide = row_x[u, s, :, cols].astype(F32).reshape(inner, experts_here, capacity, LANES)
            for e in range(experts_here):
                srt[s, e, :, cols] = wide[:, e].reshape(each, LANES).astype(jnp.bfloat16)

        chunks(part, LANES, sort)

        def product(e, start, cols_start):
            cols = pl.ds(pl.multiple_of(start + cols_start, LANES), LANES)
            return jnp.dot(srt[s, e], w_buf[e, :, cols], preferred_element_type=F32)

        for e in range(experts_here):
            def theirs(n, carry):
                at = pl.multiple_of(n * LANES, LANES)
                snd_p[u, s, e, :, pl.ds(at, LANES)] = product(e, other * half, at).astype(
                    jnp.bfloat16
                )
                return carry

            lax.fori_loop(0, half // LANES, theirs, 0)
            snd_l[u, s, e, :, :each] = lax.dot_general(
                first[e, :, my_cols], srt[s, e], (((1,), (1,)), ((), ())),
                preferred_element_type=F32,
            )
        partner_copy(u, s, 0).start()
        partner_copy(u, s, 1).start()
        for e in range(experts_here):
            def ours(n, carry):
                at = pl.multiple_of(n * LANES, LANES)
                pre[s, e, :, pl.ds(at, LANES)] = product(e, me * half, at)
                return carry

            lax.fori_loop(0, half // LANES, ours, 0)

    def back_copy(u, s):
        return remote(
            snd_b.at[u, s], rcv_b.at[u, 1 - s], bs_sem.at[u, s], br_sem.at[u, 1 - s],
            (column, other),
        )

    def back_wait(u, s):
        remote(
            snd_b.at[u, s], rcv_b.at[u, s], bs_sem.at[u, s], br_sem.at[u, s], (column, other)
        ).wait_recv()

    def slopes(u):
        for s in range(2):
            plane_wait(1, u, s)
            partner_wait(u, s, 0)
            partner_wait(u, s, 1)
            for e in range(experts_here):
                low = (snd_l[u, s, e, :, :each] + rcv_l[u, s, e, :, :each]).astype(jnp.bfloat16)
                lowb[s, e, :, :each] = low

                def one(n, carry):
                    at = pl.multiple_of(n * LANES, LANES)
                    cols = pl.ds(at, LANES)
                    adapt = lax.dot_general(
                        lowb[s, e, :, :each],
                        second[e, :, pl.ds(pl.multiple_of(me * half + at, LANES), LANES)],
                        (((0,), (0,)), ((), ())),
                        preferred_element_type=F32,
                    )
                    value = (
                        pre[s, e, :, cols]
                        + rcv_p[u, s, e, :, cols].astype(F32)
                        + ADAPTER_SCALE * adapt
                    )
                    wide = row_g[u, s, :, cols].astype(F32)
                    wide = wide.reshape(inner, experts_here, capacity, LANES)
                    given = wide[:, e].reshape(each, LANES)
                    slope[s, e, :, cols] = (given * silu_slope(value)).astype(jnp.bfloat16)
                    return carry

                lax.fori_loop(0, half // LANES, one, 0)
                snd_b[u, s, e, :, :each] = lax.dot_general(
                    second[e, :, my_hid], slope[s, e], (((1,), (1,)), ((), ())),
                    preferred_element_type=F32,
                )
            back_copy(u, s).start()

    def gradients(u):
        for s in range(2):
            for e in range(experts_here):
                acc_b[e] += jnp.dot(
                    lowb[s, e, :, :each], slope[s, e], preferred_element_type=F32
                )
        for s in range(2):
            back_wait(u, s)
            for e in range(experts_here):
                back = (snd_b[u, s, e, :, :each] + rcv_b[u, s, e, :, :each]).astype(jnp.bfloat16)
                acc_a[e] += jnp.dot(back, srt[s, e], preferred_element_type=F32)

    acc_a[...] = jnp.zeros_like(acc_a)
    acc_b[...] = jnp.zeros_like(acc_b)

    def take(k, s, kind):
        items = (0, 1) if kind == 0 else (2,)
        for item in items:
            @pl.when(jnp.logical_not(inside) | (k == 1))
            def _():
                relay(unit(k), s, item)

            @pl.when(inside & (k == 1))
            def _():
                relay(unit(2), s, item)

            if kind == 1:
                @pl.when(inside & (k == 3))
                def _():
                    relay(unit(k), s, item)

    local_x.wait()
    pack(0, z, 0)
    for item in (0, 1):
        dp_copy(item).wait_recv()
        z_send(z, 1, item, yes, yes)
    z_send(z, 0, 2, yes, yes, grd.at[:, :, my_hid])
    pack(0, z, 1)
    local_w.wait()
    local_g.wait()

    def body(k, carry):
        u = unit(k)

        @pl.when((k >= 2) & jnp.logical_not(inside))
        def _():
            def both(s, inner_carry):
                take(k, s, 0)
                pack(0, u, s)
                return inner_carry

            lax.fori_loop(0, 2, both, 0)

        @pl.when((k == 2) & inside)
        def _():
            for s in range(2):
                for item in (0, 1):
                    relay(unit(3), s, item)

        def half_unit(s, inner_carry):
            matmul(u, s)

            @pl.when((k == 0) & (s == 1))
            def _():
                dp_copy(2).wait_recv()
                z_send(z, 1, 2, yes, yes)

            @pl.when(k > 0)
            def _():
                take(k, s, 1)

            pack(1, u, s)
            return inner_carry

        lax.fori_loop(0, 2, half_unit, 0)

        @pl.when((k == 0) | (inside & (k < last)))
        def _():
            def both(s, inner_carry):
                @pl.when(k == 0)
                def _():
                    take(k + 1, s, 0)

                pack(0, unit(k + 1), s)
                return inner_carry

            lax.fori_loop(0, 2, both, 0)

        slopes(u)
        gradients(u)
        return carry

    lax.fori_loop(0, ring, body, 0)

    out_a[me] = ADAPTER_SCALE * acc_a[...]
    out_b[me] = ADAPTER_SCALE * acc_b[...]
    ends = [
        remote(ref.at[me], ref.at[me], fs_sem.at[i], fr_sem.at[i], (column, other))
        for i, ref in enumerate((out_a, out_b))
    ]
    for end in ends:
        end.start()

    def drain(u, carry):
        for s in range(2):
            for item in range(3):
                @pl.when((u <= z) & (z < last))
                def _():
                    z_copy(0, u, s, item).wait_send()

                @pl.when((u >= z) & (z > 0))
                def _():
                    z_copy(1, u, s, item).wait_send()
            for kind in range(2):
                for p in range(1, inner):
                    plane_copy(kind, u, s, p).wait_send()
            for item in range(2):
                partner_copy(u, s, item).wait_send()
            back_copy(u, s).wait_send()
        return carry

    lax.fori_loop(0, ring, drain, 0)
    for item in range(3):
        dp_copy(item).wait_send()
    for end in ends:
        end.wait()


def whole(tokens, route, gate_output_gradient, frozen_gate_weight, adapter_first, adapter_second):
    experts_here, part, hidden = frozen_gate_weight.shape
    columns = lax.axis_size("expert")
    tok_rows, width = tokens.shape
    rank = adapter_second.shape[1]
    ring, inner = RING, columns // RING
    capacity = 3 * tok_rows * route.shape[1] // (experts_here * columns)
    half, each, rows = hidden // 2, inner * capacity, inner * experts_here * capacity
    bf16 = jnp.bfloat16
    dma = pltpu.SemaphoreType.DMA
    vmem = pl.BlockSpec(memory_space=pltpu.VMEM)
    hbm = pl.BlockSpec(memory_space=pl.ANY)
    lanes = -(-each // 128) * 128
    out_a, out_b = pl.pallas_call(
        functools.partial(whole_kernel, ring, inner, capacity),
        out_shape=(
            jax.ShapeDtypeStruct((2, experts_here, rank, part), F32),
            jax.ShapeDtypeStruct((2, experts_here, rank, half), F32),
        ),
        in_specs=[hbm, hbm, vmem, hbm, vmem, vmem],
        out_specs=(vmem, vmem),
        scratch_shapes=[
            pltpu.VMEM((ring, 2, 8, tok_rows), jnp.int32),
            pltpu.VMEM((ring, 2, tok_rows, part), bf16),
            pltpu.VMEM((ring, 2, 2, tok_rows, half), bf16),
            pltpu.VMEM((ring, 2, rows, part), bf16),
            pltpu.VMEM((ring, 2, rows, half), bf16),
            pltpu.VMEM((ring, 2, rows, part), bf16),
            pltpu.VMEM((ring, 2, rows, half), bf16),
            pltpu.VMEM((experts_here, part, hidden), bf16),
            pltpu.VMEM((2, experts_here, each, part), bf16),
            pltpu.VMEM((2, experts_here, each, half), F32),
            pltpu.VMEM((2, experts_here, each, half), bf16),
            pltpu.VMEM((2, experts_here, rank, lanes), bf16),
            pltpu.VMEM((ring, 2, experts_here, each, half), bf16),
            pltpu.VMEM((ring, 2, experts_here, each, half), bf16),
            pltpu.VMEM((ring, 2, experts_here, rank, lanes), F32),
            pltpu.VMEM((ring, 2, experts_here, rank, lanes), F32),
            pltpu.VMEM((ring, 2, experts_here, rank, lanes), F32),
            pltpu.VMEM((ring, 2, experts_here, rank, lanes), F32),
            pltpu.VMEM((experts_here, rank, part), F32),
            pltpu.VMEM((experts_here, rank, half), F32),
            dma((3,)),
            dma((3,)),
            dma((3,)),
            dma((2, ring, 2, 3)),
            dma((ring, 2, 3)),
            dma((2, ring, 2, inner)),
            dma((2, ring, 2, inner)),
            dma((ring, 2, 2)),
            dma((ring, 2, 2)),
            dma((ring, 2)),
            dma((ring, 2)),
            dma((2,)),
            dma((2,)),
        ],
        compiler_params=pltpu.CompilerParams(
            collective_id=0, has_side_effects=True, vmem_limit_bytes=63 * 1024 * 1024
        ),
        name="whole",
    )(
        tokens,
        gate_output_gradient.transpose(1, 0, 2),
        route.T,
        frozen_gate_weight,
        adapter_first.transpose(0, 2, 1),
        adapter_second,
    )
    whole_a = out_a.transpose(1, 0, 3, 2).reshape(experts_here, width, rank)
    whole_b = out_b.transpose(1, 2, 0, 3).reshape(experts_here, rank, hidden)
    return (whole_a, whole_b)


def solution(mesh):
    columns, halves = mesh.shape["expert"], mesh.shape["dp"]
    fits = halves == 2 and columns % RING == 0 and columns // RING == 4
    return jax.shard_map(
        whole if fits else local,
        mesh=mesh,
        in_specs=(
            P(("expert", "dp"), None),
            P(("expert", "dp"), None),
            P(("expert", "dp"), None, None),
            P("expert", "dp", None),
            P("expert", None, None),
            P("expert", None, None),
        ),
        out_specs=(P("expert", None, None), P("expert", None, None)),
        check_vma=False,
    )
```

```python
import functools

import jax
import jax.numpy as jnp
from jax import lax
from jax.experimental import pallas as pl
from jax.experimental.pallas import tpu as pltpu
from jax.sharding import PartitionSpec as P

ADAPTER_SCALE = 2.0
RING = 4
F32 = jnp.float32


def silu_slope(gate_preactivation):
    squash = jax.nn.sigmoid(gate_preactivation)
    return squash * (1.0 + gate_preactivation * (1.0 - squash))


def dot(spec, a, b):
    return jnp.einsum(spec, a, b, preferred_element_type=F32)


def slot_codes(route, experts, capacity):
    tok_rows, top_count = route.shape
    flat_route = route.reshape(tok_rows * top_count)
    labels = jnp.arange(experts, dtype=jnp.int32)
    one_hot = (flat_route[:, None] == labels[None, :]).astype(jnp.int32)
    ranks = jnp.sum((jnp.cumsum(one_hot, axis=0) - one_hot) * one_hot, axis=1)
    return (flat_route * capacity + ranks).reshape(tok_rows, top_count)


def spread_kernel(columns, halves, own_ref, all_ref, send_sems, recv_sems):
    column, me = lax.axis_index("expert"), lax.axis_index("dp")
    total = columns * halves
    here = column * halves + me

    def peer(k):
        there = lax.rem(here + k, total)
        return (lax.div(there, halves), lax.rem(there, halves))

    barrier = pltpu.get_barrier_semaphore()

    @pl.loop(1, total)
    def _(k):
        pl.semaphore_signal(
            barrier, inc=1, device_id=peer(k), device_id_type=pl.DeviceIdType.MESH
        )

    pl.semaphore_wait(barrier, total - 1)

    def copy(k, slot):
        return pltpu.make_async_remote_copy(
            src_ref=own_ref,
            dst_ref=all_ref.at[slot],
            send_sem=send_sems.at[k],
            recv_sem=recv_sems.at[k],
            device_id=peer(k),
            device_id_type=pl.DeviceIdType.MESH,
        )

    @pl.loop(1, total)
    def _(k):
        copy(k, here).start()

    all_ref[here] = own_ref[...]

    @pl.loop(1, total)
    def _(k):
        copy(k, lax.rem(here + total - k, total)).wait()


def spread(value, columns, halves):
    total = columns * halves
    return pl.pallas_call(
        functools.partial(spread_kernel, columns, halves),
        out_shape=jax.ShapeDtypeStruct((total, *value.shape), value.dtype),
        in_specs=[pl.BlockSpec(memory_space=pltpu.VMEM)],
        out_specs=pl.BlockSpec(memory_space=pltpu.VMEM),
        scratch_shapes=[
            pltpu.SemaphoreType.DMA((total,)),
            pltpu.SemaphoreType.DMA((total,)),
        ],
        compiler_params=pltpu.CompilerParams(collective_id=0, has_side_effects=True),
        name="spread",
    )(value)


def local(tokens, route, gate_output_gradient, frozen_gate_weight, adapter_first, adapter_second):
    experts_here, part, hidden = frozen_gate_weight.shape
    columns, halves = lax.axis_size("expert"), lax.axis_size("dp")
    experts = experts_here * columns
    tok_rows, width = tokens.shape
    top_count = route.shape[1]
    capacity = 3 * tok_rows * top_count // experts
    hidden_part = hidden // halves
    ring = RING if columns % RING == 0 else 1
    inner = columns // ring
    column, me = lax.axis_index("expert"), lax.axis_index("dp")
    outer_at, inner_at = column // inner, column % inner

    codes = slot_codes(route, experts, capacity)
    all_codes = spread(codes.T, columns, halves).transpose(0, 2, 1).reshape(
        columns, halves, tok_rows, top_count
    )

    def piece(target):
        parts = [lax.dynamic_slice_in_dim(tokens, target * part, part, 1)]
        for k in range(top_count):
            parts.append(
                lax.dynamic_slice_in_dim(
                    gate_output_gradient[:, k], target * hidden_part, hidden_part, 1
                )
            )
        return jnp.concatenate(parts, axis=1)

    def dp_shift(value, k):
        return lax.ppermute(value, "dp", [(i, (i + k) % halves) for i in range(halves)])

    def dp_sum(value):
        total = value
        for k in range(1, halves):
            total = total + dp_shift(jnp.roll(value, k, axis=1), k)
        return total

    streams = [(piece(me)[None], [0])]
    if halves > 1:
        others = [dp_shift(piece((me + k) % halves), k) for k in range(1, halves)]
        streams.append((jnp.stack(others), list(range(1, halves))))

    around = [(i, (i + inner) % columns) for i in range(columns)]
    first_part = lax.dynamic_slice_in_dim(adapter_first, me * part, part, 1)
    second_part = lax.dynamic_slice_in_dim(adapter_second, me * hidden_part, hidden_part, 2)
    group = experts_here * capacity
    places = (
        (outer_at * inner + (inner_at + jnp.arange(inner, dtype=jnp.int32)) % inner)[:, None]
        * group
        + jnp.arange(group, dtype=jnp.int32)[None, :]
    ).reshape(inner * group)

    grad_a, grad_b = 0.0, 0.0
    blocks = [stream[0] for stream in streams]
    for step in range(ring):
        source = (outer_at + ring - step) % ring * inner + inner_at
        step_codes = lax.dynamic_index_in_dim(all_codes, source, 0, keepdims=False)
        following, step_rows = [], []
        for (_, shifts), block in zip(streams, blocks):
            if step < ring - 1:
                following.append(lax.ppermute(block, "expert", around))
            count = len(shifts)
            own_codes = jnp.stack(
                [
                    lax.dynamic_index_in_dim(step_codes, (me + halves - k) % halves, 0, keepdims=False)
                    for k in shifts
                ]
            )
            picks = [
                (own_codes[:, None, :, k] == places[None, :, None]).astype(jnp.bfloat16)
                for k in range(top_count)
            ]
            packed_x = dot("mrt,mtw->mrw", sum(picks[1:], picks[0]), block[:, :, :part])
            packed_g = sum(
                dot(
                    "mrt,mtw->mrw",
                    picks[k],
                    block[:, :, part + k * hidden_part : part + (k + 1) * hidden_part],
                )
                for k in range(top_count)
            )
            packed = jnp.concatenate(
                [packed_x.astype(jnp.bfloat16), packed_g.astype(jnp.bfloat16)], axis=2
            ).reshape(count, inner, group, part + hidden_part)
            arrived = [packed[:, 0]]
            for j in range(1, inner):
                pairs = [
                    (o * inner + i, o * inner + (i + j) % inner)
                    for o in range(ring)
                    for i in range(inner)
                ]
                arrived.append(lax.ppermute(packed[:, j], "expert", pairs))
            step_rows.append(
                jnp.stack(arrived, 1).reshape(count, inner, experts_here, capacity, -1)
            )
        rows = jnp.concatenate(step_rows, axis=0).transpose(2, 0, 1, 3, 4)
        rows = rows.reshape(experts_here, halves, inner * capacity, -1)
        rows_x, rows_g = rows[..., :part], rows[..., part:]
        partial = dot("ednw,ewf->ednf", rows_x, frozen_gate_weight)
        low = dp_sum(dot("ednw,ewr->ednr", rows_x, first_part)).astype(jnp.bfloat16)

        def take(target):
            return lax.dynamic_slice_in_dim(partial, target * hidden_part, hidden_part, 3)

        preact = take(me) + ADAPTER_SCALE * dot("ednr,erf->ednf", low, second_part)
        for k in range(1, halves):
            sent = jnp.roll(take((me + k) % halves).astype(jnp.bfloat16), k, axis=1)
            preact = preact + dp_shift(sent, k).astype(F32)
        slope = (rows_g.astype(F32) * silu_slope(preact)).astype(jnp.bfloat16)
        back = dp_sum(dot("ednf,erf->ednr", slope, second_part)).astype(jnp.bfloat16)
        grad_b = grad_b + dot("ednr,ednf->erf", low, slope)
        grad_a = grad_a + dot("ednr,ednw->erw", back, rows_x)
        blocks = following

    joined = ADAPTER_SCALE * jnp.concatenate([grad_a, grad_b], axis=2)
    pieces = [joined] + [dp_shift(joined, k) for k in range(1, halves)]
    stacked = jnp.stack(pieces[::-1])
    whole = jnp.roll(stacked, me + 1, axis=0)
    whole_a = whole[:, :, :, :part].transpose(1, 0, 3, 2).reshape(experts_here, width, -1)
    whole_b = whole[:, :, :, part:].transpose(1, 2, 0, 3).reshape(experts_here, -1, hidden)
    return (whole_a, whole_b)


MESH = pl.DeviceIdType.MESH
LANES = 256


def chunks(extent, size, body):
    def step(n, carry):
        body(pl.ds(pl.multiple_of(n * size, size), size))
        return carry

    lax.fori_loop(0, extent // size, step, 0)


def whole_kernel(
    ring, inner, capacity,
    tok, grd, route, wgt, first, second,
    out_a, out_b,
    blk_c, blk_x, blk_g, edge_g, stg_x, stg_g, row_x, row_g, w_buf, srt, pre, slope, lowb,
    snd_p, rcv_p, snd_l, rcv_l, snd_b, rcv_b, acc_a, acc_b, got_a, got_b, end_a, end_b,
    loc_sem, dps_sem, dpr_sem, zs_sem, zr_sem, gs_sem, gr_sem, ps_sem, pr_sem, qs_sem, qr_sem, bs_sem, br_sem,
    fs_sem, fr_sem,
):
    column, me = lax.axis_index("expert"), lax.axis_index("dp")
    z, p0 = column // inner, column % inner
    other = 1 - me
    experts_here, part, hidden = w_buf.shape
    half = hidden // 2
    tok_rows = tok.shape[0]
    group = experts_here * capacity
    total_rows = inner * group
    each = inner * capacity
    experts = experts_here * inner * ring
    last = ring - 1
    inside = (z > 0) & (z < last)

    def unit(k):
        near = jnp.where(inside, jnp.where(k == 1, 2, jnp.where(k == 2, 0, k)), k)
        flipped = jnp.where(z < ring // 2, near, last - near)
        return jnp.where(k == 0, z, flipped)

    barrier = pltpu.get_barrier_semaphore()

    def greet(device):
        pl.semaphore_signal(barrier, inc=1, device_id=device, device_id_type=MESH)

    for p in range(1, inner):
        greet((z * inner + (p0 + p) % inner, me))
    greet((column, other))

    @pl.when(z > 0)
    def _():
        greet((column - inner, me))

    @pl.when(z < last)
    def _():
        greet((column + inner, me))

    pl.semaphore_wait(
        barrier, inner + jnp.where(z > 0, 1, 0) + jnp.where(z < last, 1, 0)
    )

    my_cols = pl.ds(pl.multiple_of(me * part, part), part)
    its_cols = pl.ds(pl.multiple_of(other * part, part), part)
    my_hid = pl.ds(pl.multiple_of(me * half, half), half)
    its_hid = pl.ds(pl.multiple_of(other * half, half), half)
    blocks = (blk_c, blk_x, blk_g)
    core = p0 % 2
    far_first = (2, 3 - 2 * core, 1 + 2 * core)
    ordered = tuple(zip((*far_first, 0), (False, False, True, True)))

    def remote(src, dst, send, recv, device):
        return pltpu.make_async_remote_copy(
            src_ref=src, dst_ref=dst, send_sem=send, recv_sem=recv,
            device_id=device, device_id_type=MESH,
        )

    def arrived(ref, sem):
        remote(ref, ref, fs_sem.at[0], sem, (column, other)).wait_recv()

    def sent(ref, sem):
        remote(ref, ref, sem, fr_sem.at[0], (column, other)).wait_send()

    local_x = pltpu.make_async_copy(tok.at[:, my_cols], blk_x.at[z, 0], loc_sem.at[0])
    local_g = pltpu.make_async_copy(grd.at[:, :, my_hid], blk_g.at[z, 0], loc_sem.at[1])
    local_w = pltpu.make_async_copy(wgt, w_buf, loc_sem.at[2])

    def dp_copy(item):
        src = (blk_c.at[z, 0], tok.at[:, its_cols], grd.at[:, :, its_hid])[item]
        return remote(
            src, blocks[item].at[z, 1], dps_sem.at[item], dpr_sem.at[item], (column, other)
        )

    def z_copy(way, u, s, item, src=None):
        step = inner if way == 0 else -inner
        dst = blocks[item].at[u, s]
        return remote(
            dst if src is None else src, dst,
            zs_sem.at[way, item], zr_sem.at[u, s, item], (column + step, me),
        )

    def rows_of(p):
        return pl.ds(pl.multiple_of((p0 + p) % inner * group, group), group)

    def z_piece(way, u, s, p, near_side):
        step = inner if way == 0 else -inner
        return remote(
            edge_g.at[u, s, rows_of(p), :], stg_g.at[u, s, rows_of(p), :],
            gs_sem.at[0], gr_sem.at[u, s, 0 if near_side else 1], (column + step, me),
        )

    def to_end(way):
        return (z == last - 1) if way == 0 else (z == 1)

    def z_send(u, s, item, up, down, src=None):
        for way, on in ((0, up & (z < last)), (1, down & (z > 0))):
            if item < 2:
                @pl.when(on)
                def _():
                    z_copy(way, u, s, item, src).start()
            else:
                @pl.when(on & jnp.logical_not(to_end(way)))
                def _():
                    z_copy(way, u, s, item, src).start()

                @pl.when(on & to_end(way))
                def _():
                    fill(1, edge_g, u, s, last if way == 0 else 0)
                    for p, near_side in ordered:
                        z_piece(way, u, s, p, near_side).start()

    def relay(u, s, item):
        z_copy(0, u, s, item).wait_recv()
        z_send(u, s, item, u < z, u > z)

    yes = z >= 0
    local_x.start()
    dp_copy(1).start()
    z_send(z, 0, 1, yes, yes, tok.at[:, my_cols])
    local_g.start()

    labels = lax.broadcasted_iota(jnp.int32, (experts, tok_rows), 0)
    ones = [jnp.where(route[k : k + 1, :] == labels, 1.0, 0.0) for k in range(2)]
    earlier = jnp.where(
        lax.broadcasted_iota(jnp.int32, (tok_rows, tok_rows), 0)
        < lax.broadcasted_iota(jnp.int32, (tok_rows, tok_rows), 1),
        1.0,
        0.0,
    ).astype(jnp.bfloat16)
    before = [
        jnp.dot(one.astype(jnp.bfloat16), earlier, preferred_element_type=F32) for one in ones
    ]
    before[1] = before[1] + jnp.sum(ones[0], axis=1, keepdims=True)
    base = lax.broadcasted_iota(jnp.int32, (experts, tok_rows), 0).astype(F32) * capacity
    for k in range(2):
        code = jnp.sum(ones[k] * (before[k] + base), axis=0, keepdims=True)
        blk_c[z, 0, k : k + 1, :] = code.astype(jnp.int32)
    dp_copy(0).start()
    dp_copy(2).start()
    z_send(z, 0, 0, yes, yes)
    local_w.start()

    def plane_copy(kind, u, s, p):
        stage, rows = ((stg_x, row_x), (stg_g, row_g))[kind]
        peer = (p0 + p) % inner
        return remote(
            stage.at[u, s, pl.ds(pl.multiple_of(peer * group, group), group), :],
            rows.at[u, s, pl.ds(pl.multiple_of(p0 * group, group), group), :],
            ps_sem.at[kind], pr_sem.at[kind, u, s], (z * inner + peer, me),
        )

    def plane_wait(kind, u, s):
        rows = (row_x, row_g)[kind]
        arrived(rows.at[u, s, pl.ds(0, (inner - 1) * group), :], pr_sem.at[kind, u, s])

    def fill(kind, stage, u, s, plane):
        place = plane * total_rows + lax.broadcasted_iota(
            jnp.int32, (total_rows, tok_rows), 0
        )
        picks = [blk_c[u, s, k : k + 1, :] == place for k in range(2)]
        if kind == 0:
            chosen = jnp.where(picks[0] | picks[1], 1.0, 0.0).astype(jnp.bfloat16)
        else:
            chosen = jnp.concatenate(
                [jnp.where(pick, 1.0, 0.0).astype(jnp.bfloat16) for pick in picks], axis=1
            )

        def one(cols):
            if kind == 0:
                block = blk_x[u, s, :, cols]
            else:
                block = blk_g[u, s, :, :, cols].reshape(2 * tok_rows, LANES)
            stage[u, s, :, cols] = jnp.dot(
                chosen, block, preferred_element_type=F32
            ).astype(jnp.bfloat16)

        chunks(stage.shape[-1], LANES, one)

    def pack(kind, u, s):
        stage, rows = ((stg_x, row_x), (stg_g, row_g))[kind]
        fill(kind, stage, u, s, z)
        for p in far_first:
            plane_copy(kind, u, s, p).start()
        rows[u, s, rows_of(0), :] = stage[u, s, rows_of(0), :]

    def pass_on(u, s):
        pair = stg_g.at[u, s, pl.ds(0, 2 * group), :]
        for i, peers in ((1, far_first[:2]), (0, far_first[2:])):
            arrived(pair, gr_sem.at[u, s, i])
            for p in peers:
                plane_copy(1, u, s, p).start()
        row_g[u, s, rows_of(0), :] = stg_g[u, s, rows_of(0), :]

    def partner_copy(u, s, item):
        src, dst = ((snd_p, rcv_p), (snd_l, rcv_l))[item]
        return remote(
            src.at[u, s], dst.at[u, 1 - s], qs_sem.at[item], qr_sem.at[u, 1 - s, item],
            (column, other),
        )

    def partner_wait(u, s, item):
        src, dst = ((snd_p, rcv_p), (snd_l, rcv_l))[item]
        remote(
            src.at[u, s], dst.at[u, s], qs_sem.at[item], qr_sem.at[u, s, item],
            (column, other),
        ).wait_recv()

    def matmul(u, s, par):
        plane_wait(0, u, s)

        def sort(cols):
            wide = row_x[u, s, :, cols].astype(F32).reshape(inner, experts_here, capacity, LANES)
            for e in range(experts_here):
                srt[par, s, e, :, cols] = wide[:, e].reshape(each, LANES).astype(jnp.bfloat16)

        chunks(part, LANES, sort)

        def product(e, cols):
            return jnp.dot(srt[par, s, e], w_buf[e, :, cols], preferred_element_type=F32)

        for e in range(experts_here):
            snd_p[u, s, e] = product(e, its_hid).astype(jnp.bfloat16)
            snd_l[u, s, e, :, :each] = lax.dot_general(
                first[e, :, my_cols], srt[par, s, e], (((1,), (1,)), ((), ())),
                preferred_element_type=F32,
            )
        partner_copy(u, s, 0).start()
        partner_copy(u, s, 1).start()
        for e in range(experts_here):
            pre[par, s, e] = product(e, my_hid)

    def back_copy(u, s):
        return remote(
            snd_b.at[u, s], rcv_b.at[u, 1 - s], bs_sem.at[0], br_sem.at[u, 1 - s],
            (column, other),
        )

    def back_wait(u, s):
        remote(
            snd_b.at[u, s], rcv_b.at[u, s], bs_sem.at[0], br_sem.at[u, s], (column, other)
        ).wait_recv()

    def act(u, par):
        for s in range(2):
            partner_wait(u, s, 0)
            partner_wait(u, s, 1)
            for e in range(experts_here):
                low = (snd_l[u, s, e, :, :each] + rcv_l[u, s, e, :, :each]).astype(jnp.bfloat16)
                lowb[par, s, e, :, :each] = low

                def one(n, carry):
                    at = pl.multiple_of(n * LANES, LANES)
                    cols = pl.ds(at, LANES)
                    adapt = lax.dot_general(
                        lowb[par, s, e, :, :each],
                        second[e, :, pl.ds(pl.multiple_of(me * half + at, LANES), LANES)],
                        (((0,), (0,)), ((), ())),
                        preferred_element_type=F32,
                    )
                    value = (
                        pre[par, s, e, :, cols]
                        + rcv_p[u, s, e, :, cols].astype(F32)
                        + ADAPTER_SCALE * adapt
                    )
                    pre[par, s, e, :, cols] = silu_slope(value)
                    return carry

                lax.fori_loop(0, half // LANES, one, 0)

    def slopes(u, par):
        for s in range(2):
            plane_wait(1, u, s)

            def one(n, carry):
                cols = pl.ds(pl.multiple_of(n * LANES, LANES), LANES)
                wide = row_g[u, s, :, cols].astype(F32)
                wide = wide.reshape(inner, experts_here, capacity, LANES)
                for e in range(experts_here):
                    given = wide[:, e].reshape(each, LANES)
                    slope[s, e, :, cols] = (given * pre[par, s, e, :, cols]).astype(jnp.bfloat16)
                return carry

            lax.fori_loop(0, half // LANES, one, 0)
            for e in range(experts_here):
                snd_b[u, s, e, :, :each] = lax.dot_general(
                    second[e, :, my_hid], slope[s, e], (((1,), (1,)), ((), ())),
                    preferred_element_type=F32,
                )
            back_copy(u, s).start()

    def gradients(u, par, late, final):
        for s in range(2):
            for e in range(experts_here):
                acc_b[late, e] += jnp.dot(
                    lowb[par, s, e, :, :each], slope[s, e], preferred_element_type=F32
                )

        @pl.when(final)
        def _():
            end_b[0] = acc_b[1].astype(jnp.bfloat16)
            ends[1].start()

        for s in range(2):
            back_wait(u, s)
            for e in range(experts_here):
                back = (snd_b[u, s, e, :, :each] + rcv_b[u, s, e, :, :each]).astype(jnp.bfloat16)
                acc_a[late, e] += jnp.dot(back, srt[par, s, e], preferred_element_type=F32)

        @pl.when(final)
        def _():
            end_a[0] = acc_a[1].astype(jnp.bfloat16)
            ends[0].start()

    ends = [
        remote(ref.at[0], ref.at[1], fs_sem.at[2 + i], fr_sem.at[2 + i], (column, other))
        for i, ref in enumerate((end_a, end_b))
    ]
    firsts = [
        remote(src.at[0], dst, fs_sem.at[i], fr_sem.at[i], (column, other))
        for i, (src, dst) in enumerate(((acc_a, got_a), (acc_b, got_b)))
    ]
    acc_a[...] = jnp.zeros_like(acc_a)
    acc_b[...] = jnp.zeros_like(acc_b)

    def relay_x(u, s):
        for item in (0, 1):
            relay(u, s, item)

    def twice(step):
        def run(s, carry):
            step(s)
            return carry

        lax.fori_loop(0, 2, run, 0)

    local_g.wait()
    z_send(z, 0, 2, yes, yes, grd.at[:, :, my_hid])
    local_x.wait()
    pack(0, z, 0)
    for item in (0, 1):
        dp_copy(item).wait_recv()
        z_send(z, 1, item, yes, yes)
    pack(0, z, 1)
    local_w.wait()
    at_end = jnp.logical_not(inside)

    def when(condition, step, *args):
        @pl.when(condition)
        def _():
            step(*args)

    def bring_x(k, s):
        relay_x(unit(k), s)
        pack(0, unit(k), s)

    def first_x(s):
        relay_x(unit(1), s)
        when(inside, relay_x, unit(2), s)
        pack(0, unit(1), s)

    def near_g():
        relay_x(unit(3), 1)
        near = unit(1)
        twice(lambda i: z_send(near, i, 2, near < z, near > z))

    def bring_g(k, s):
        relay(unit(k), s, 2)
        pack(1, unit(k), s)

    def second_g(s):
        z_copy(0, unit(1), s, 2).wait_recv()
        relay(unit(2), s, 2)
        pack(1, unit(1), s)

    def own_g(s):
        @pl.when(s == 1)
        def _():
            dp_copy(2).wait_recv()
            z_send(z, 1, 2, yes, yes)

        pack(1, z, s)

    def finish(kk, inner_carry):
        when((kk == 2) & at_end, pass_on, unit(3), 0)
        when(inside | (kk < 2), act, unit(kk), kk % 2)
        slopes(unit(kk), kk % 2)

        @pl.when((kk == 2) & at_end)
        def _():
            act(unit(3), 1)
            pass_on(unit(3), 1)

        gradients(unit(kk), kk % 2, jnp.where(kk >= 2, 1, 0), kk == 3)

        @pl.when(kk == 1)
        def _():
            for end in firsts:
                end.start()

        return inner_carry

    def body(b, carry):
        k, s = b // 2, b % 2
        when((b == 1) | (b == 2), first_x, b - 1)
        when((b == 4) & at_end, bring_x, 2, 1)
        when(((b == 5) | (b == 6)) & at_end, bring_x, 3, b - 5)
        when((b == 7) & at_end, pass_on, unit(2), 0)
        when((b == 7) & at_end, act, unit(2), 0)
        when(((b == 3) | (b == 4)) & inside, pack, 0, unit(2), b - 3)
        when((b == 4) & inside, relay_x, unit(3), 0)
        when(((b == 5) | (b == 6)) & inside, pack, 0, unit(3), b - 5)
        matmul(unit(k), s, k % 2)
        when(k == 0, own_g, s)
        when((k == 1) & at_end, pass_on, unit(1), s)
        when((b == 3) & at_end, bring_x, 2, 0)
        when((k == 1) & inside, second_g, s)
        when((b == 4) & inside, near_g)
        when((k == 2) & inside, pack, 1, unit(2), s)
        when((k == 3) & inside, bring_g, 3, s)
        when((b == 7) & at_end, pass_on, unit(2), 1)
        begin = jnp.where(
            b == 2,
            0,
            jnp.where(
                b == jnp.where(inside, 4, 3),
                1,
                jnp.where(b == jnp.where(inside, 6, 7), 2, jnp.where(b == 7, 3, 4)),
            ),
        )
        stop = jnp.where(begin == 4, 4, jnp.where(b == 7, 4, begin + 1))
        lax.fori_loop(begin, stop, finish, 0)
        return carry

    lax.fori_loop(0, 2 * ring, body, 0)
    out_a[:, :, my_cols] = acc_a[0] + end_a[0].astype(F32)
    out_b[:, :, my_hid] = acc_b[0] + end_b[0].astype(F32)

    for item, ref in enumerate(blocks):
        for n in range(1, ring):
            up, down = z == n - 1, z == ring - n
            if item == 2:
                up, down = up & (z < last - 1), down & (z > 1)
            when(up, sent, ref.at[pl.ds(0, n)], zs_sem.at[0, item])
            when(down, sent, ref.at[pl.ds(0, n)], zs_sem.at[1, item])
    when(inside, sent, edge_g.at[pl.ds(0, last)], gs_sem.at[0])
    share = ring * (inner - 1) // inner
    sent(stg_x.at[pl.ds(0, share)], ps_sem.at[0])
    sent(stg_g.at[pl.ds(0, share)], ps_sem.at[1])
    sent(snd_p, qs_sem.at[0])
    sent(snd_l, qs_sem.at[1])
    sent(snd_b, bs_sem.at[0])
    for item in range(3):
        dp_copy(item).wait_send()
    for end in firsts:
        end.wait()
    for end in ends:
        end.wait()
    out_a[:, :, its_cols] = got_a[...] + end_a[1].astype(F32)
    out_b[:, :, its_hid] = got_b[...] + end_b[1].astype(F32)


def scale_kernel(in_a, in_b, out_a, out_b):
    out_a[...] = ADAPTER_SCALE * in_a[...]
    out_b[...] = ADAPTER_SCALE * in_b[...]


def whole(tokens, route, gate_output_gradient, frozen_gate_weight, adapter_first, adapter_second):
    experts_here, part, hidden = frozen_gate_weight.shape
    columns = lax.axis_size("expert")
    tok_rows, width = tokens.shape
    rank = adapter_second.shape[1]
    ring, inner = RING, columns // RING
    capacity = 3 * tok_rows * route.shape[1] // (experts_here * columns)
    half, each, rows = hidden // 2, inner * capacity, inner * experts_here * capacity
    bf16 = jnp.bfloat16
    dma = pltpu.SemaphoreType.DMA
    vmem = pl.BlockSpec(memory_space=pltpu.VMEM)
    hbm = pl.BlockSpec(memory_space=pl.ANY)
    lanes = -(-each // 128) * 128
    out_a, out_b = pl.pallas_call(
        functools.partial(whole_kernel, ring, inner, capacity),
        out_shape=(
            jax.ShapeDtypeStruct((experts_here, rank, width), F32),
            jax.ShapeDtypeStruct((experts_here, rank, hidden), F32),
        ),
        in_specs=[hbm, hbm, vmem, hbm, vmem, vmem],
        out_specs=(vmem, vmem),
        scratch_shapes=[
            pltpu.VMEM((ring, 2, 2, tok_rows), jnp.int32),
            pltpu.VMEM((ring, 2, tok_rows, part), bf16),
            pltpu.VMEM((ring, 2, 2, tok_rows, half), bf16),
            pltpu.VMEM((ring, 2, rows, half), bf16),
            pltpu.VMEM((ring, 2, rows, part), bf16),
            pltpu.VMEM((ring, 2, rows, half), bf16),
            pltpu.VMEM((ring, 2, rows, part), bf16),
            pltpu.VMEM((ring, 2, rows, half), bf16),
            pltpu.VMEM((experts_here, part, hidden), bf16),
            pltpu.VMEM((2, 2, experts_here, each, part), bf16),
            pltpu.VMEM((2, 2, experts_here, each, half), F32),
            pltpu.VMEM((2, experts_here, each, half), bf16),
            pltpu.VMEM((2, 2, experts_here, rank, lanes), bf16),
            pltpu.VMEM((ring, 2, experts_here, each, half), bf16),
            pltpu.VMEM((ring, 2, experts_here, each, half), bf16),
            pltpu.VMEM((ring, 2, experts_here, rank, lanes), F32),
            pltpu.VMEM((ring, 2, experts_here, rank, lanes), F32),
            pltpu.VMEM((ring, 2, experts_here, rank, lanes), F32),
            pltpu.VMEM((ring, 2, experts_here, rank, lanes), F32),
            pltpu.VMEM((2, experts_here, rank, part), F32),
            pltpu.VMEM((2, experts_here, rank, half), F32),
            pltpu.VMEM((experts_here, rank, part), F32),
            pltpu.VMEM((experts_here, rank, half), F32),
            pltpu.VMEM((2, experts_here, rank, part), bf16),
            pltpu.VMEM((2, experts_here, rank, half), bf16),
            dma((3,)),
            dma((3,)),
            dma((3,)),
            dma((2, 3)),
            dma((ring, 2, 3)),
            dma((1,)),
            dma((ring, 2, 2)),
            dma((2,)),
            dma((2, ring, 2)),
            dma((2,)),
            dma((ring, 2, 2)),
            dma((1,)),
            dma((ring, 2)),
            dma((4,)),
            dma((4,)),
        ],
        compiler_params=pltpu.CompilerParams(
            collective_id=0, has_side_effects=True, vmem_limit_bytes=58 * 1024 * 1024
        ),
        name="whole",
    )(
        tokens,
        gate_output_gradient.transpose(1, 0, 2),
        route.T,
        frozen_gate_weight,
        adapter_first.transpose(0, 2, 1),
        adapter_second,
    )
    scaled_a, scaled_b = pl.pallas_call(
        scale_kernel,
        out_shape=(
            jax.ShapeDtypeStruct(out_a.shape, F32),
            jax.ShapeDtypeStruct(out_b.shape, F32),
        ),
        in_specs=[vmem, vmem],
        out_specs=(vmem, vmem),
        name="scale",
    )(out_a, out_b)
    return (scaled_a.transpose(0, 2, 1), scaled_b)


def solution(mesh):
    columns, halves = mesh.shape["expert"], mesh.shape["dp"]
    fits = halves == 2 and columns % RING == 0 and columns // RING == 4
    return jax.shard_map(
        whole if fits else local,
        mesh=mesh,
        in_specs=(
            P(("expert", "dp"), None),
            P(("expert", "dp"), None),
            P(("expert", "dp"), None, None),
            P("expert", "dp", None),
            P("expert", None, None),
            P("expert", None, None),
        ),
        out_specs=(P("expert", None, None), P("expert", None, None)),
        check_vma=False,
    )
```

```python
import functools

import jax
import jax.numpy as jnp
from jax import lax
from jax.experimental import pallas as pl
from jax.experimental.pallas import tpu as pltpu
from jax.sharding import PartitionSpec as P

ADAPTER_SCALE = 2.0
RING = 4
F32 = jnp.float32


def silu_slope(gate_preactivation):
    squash = jax.nn.sigmoid(gate_preactivation)
    return squash * (1.0 + gate_preactivation * (1.0 - squash))


def dot(spec, a, b):
    return jnp.einsum(spec, a, b, preferred_element_type=F32)


def slot_codes(route, experts, capacity):
    tok_rows, top_count = route.shape
    flat_route = route.reshape(tok_rows * top_count)
    labels = jnp.arange(experts, dtype=jnp.int32)
    one_hot = (flat_route[:, None] == labels[None, :]).astype(jnp.int32)
    ranks = jnp.sum((jnp.cumsum(one_hot, axis=0) - one_hot) * one_hot, axis=1)
    return (flat_route * capacity + ranks).reshape(tok_rows, top_count)


def spread_kernel(columns, halves, own_ref, all_ref, send_sems, recv_sems):
    column, me = lax.axis_index("expert"), lax.axis_index("dp")
    total = columns * halves
    here = column * halves + me

    def peer(k):
        there = lax.rem(here + k, total)
        return (lax.div(there, halves), lax.rem(there, halves))

    barrier = pltpu.get_barrier_semaphore()

    @pl.loop(1, total)
    def _(k):
        pl.semaphore_signal(
            barrier, inc=1, device_id=peer(k), device_id_type=pl.DeviceIdType.MESH
        )

    pl.semaphore_wait(barrier, total - 1)

    def copy(k, slot):
        return pltpu.make_async_remote_copy(
            src_ref=own_ref,
            dst_ref=all_ref.at[slot],
            send_sem=send_sems.at[k],
            recv_sem=recv_sems.at[k],
            device_id=peer(k),
            device_id_type=pl.DeviceIdType.MESH,
        )

    @pl.loop(1, total)
    def _(k):
        copy(k, here).start()

    all_ref[here] = own_ref[...]

    @pl.loop(1, total)
    def _(k):
        copy(k, lax.rem(here + total - k, total)).wait()


def spread(value, columns, halves):
    total = columns * halves
    return pl.pallas_call(
        functools.partial(spread_kernel, columns, halves),
        out_shape=jax.ShapeDtypeStruct((total, *value.shape), value.dtype),
        in_specs=[pl.BlockSpec(memory_space=pltpu.VMEM)],
        out_specs=pl.BlockSpec(memory_space=pltpu.VMEM),
        scratch_shapes=[
            pltpu.SemaphoreType.DMA((total,)),
            pltpu.SemaphoreType.DMA((total,)),
        ],
        compiler_params=pltpu.CompilerParams(collective_id=0, has_side_effects=True),
        name="spread",
    )(value)


def local(tokens, route, gate_output_gradient, frozen_gate_weight, adapter_first, adapter_second):
    experts_here, part, hidden = frozen_gate_weight.shape
    columns, halves = lax.axis_size("expert"), lax.axis_size("dp")
    experts = experts_here * columns
    tok_rows, width = tokens.shape
    top_count = route.shape[1]
    capacity = 3 * tok_rows * top_count // experts
    hidden_part = hidden // halves
    ring = RING if columns % RING == 0 else 1
    inner = columns // ring
    column, me = lax.axis_index("expert"), lax.axis_index("dp")
    outer_at, inner_at = column // inner, column % inner

    codes = slot_codes(route, experts, capacity)
    all_codes = spread(codes.T, columns, halves).transpose(0, 2, 1).reshape(
        columns, halves, tok_rows, top_count
    )

    def piece(target):
        parts = [lax.dynamic_slice_in_dim(tokens, target * part, part, 1)]
        for k in range(top_count):
            parts.append(
                lax.dynamic_slice_in_dim(
                    gate_output_gradient[:, k], target * hidden_part, hidden_part, 1
                )
            )
        return jnp.concatenate(parts, axis=1)

    def dp_shift(value, k):
        return lax.ppermute(value, "dp", [(i, (i + k) % halves) for i in range(halves)])

    def dp_sum(value):
        total = value
        for k in range(1, halves):
            total = total + dp_shift(jnp.roll(value, k, axis=1), k)
        return total

    streams = [(piece(me)[None], [0])]
    if halves > 1:
        others = [dp_shift(piece((me + k) % halves), k) for k in range(1, halves)]
        streams.append((jnp.stack(others), list(range(1, halves))))

    around = [(i, (i + inner) % columns) for i in range(columns)]
    first_part = lax.dynamic_slice_in_dim(adapter_first, me * part, part, 1)
    second_part = lax.dynamic_slice_in_dim(adapter_second, me * hidden_part, hidden_part, 2)
    group = experts_here * capacity
    places = (
        (outer_at * inner + (inner_at + jnp.arange(inner, dtype=jnp.int32)) % inner)[:, None]
        * group
        + jnp.arange(group, dtype=jnp.int32)[None, :]
    ).reshape(inner * group)

    grad_a, grad_b = 0.0, 0.0
    blocks = [stream[0] for stream in streams]
    for step in range(ring):
        source = (outer_at + ring - step) % ring * inner + inner_at
        step_codes = lax.dynamic_index_in_dim(all_codes, source, 0, keepdims=False)
        following, step_rows = [], []
        for (_, shifts), block in zip(streams, blocks):
            if step < ring - 1:
                following.append(lax.ppermute(block, "expert", around))
            count = len(shifts)
            own_codes = jnp.stack(
                [
                    lax.dynamic_index_in_dim(step_codes, (me + halves - k) % halves, 0, keepdims=False)
                    for k in shifts
                ]
            )
            picks = [
                (own_codes[:, None, :, k] == places[None, :, None]).astype(jnp.bfloat16)
                for k in range(top_count)
            ]
            packed_x = dot("mrt,mtw->mrw", sum(picks[1:], picks[0]), block[:, :, :part])
            packed_g = sum(
                dot(
                    "mrt,mtw->mrw",
                    picks[k],
                    block[:, :, part + k * hidden_part : part + (k + 1) * hidden_part],
                )
                for k in range(top_count)
            )
            packed = jnp.concatenate(
                [packed_x.astype(jnp.bfloat16), packed_g.astype(jnp.bfloat16)], axis=2
            ).reshape(count, inner, group, part + hidden_part)
            arrived = [packed[:, 0]]
            for j in range(1, inner):
                pairs = [
                    (o * inner + i, o * inner + (i + j) % inner)
                    for o in range(ring)
                    for i in range(inner)
                ]
                arrived.append(lax.ppermute(packed[:, j], "expert", pairs))
            step_rows.append(
                jnp.stack(arrived, 1).reshape(count, inner, experts_here, capacity, -1)
            )
        rows = jnp.concatenate(step_rows, axis=0).transpose(2, 0, 1, 3, 4)
        rows = rows.reshape(experts_here, halves, inner * capacity, -1)
        rows_x, rows_g = rows[..., :part], rows[..., part:]
        partial = dot("ednw,ewf->ednf", rows_x, frozen_gate_weight)
        low = dp_sum(dot("ednw,ewr->ednr", rows_x, first_part)).astype(jnp.bfloat16)

        def take(target):
            return lax.dynamic_slice_in_dim(partial, target * hidden_part, hidden_part, 3)

        preact = take(me) + ADAPTER_SCALE * dot("ednr,erf->ednf", low, second_part)
        for k in range(1, halves):
            sent = jnp.roll(take((me + k) % halves).astype(jnp.bfloat16), k, axis=1)
            preact = preact + dp_shift(sent, k).astype(F32)
        slope = (rows_g.astype(F32) * silu_slope(preact)).astype(jnp.bfloat16)
        back = dp_sum(dot("ednf,erf->ednr", slope, second_part)).astype(jnp.bfloat16)
        grad_b = grad_b + dot("ednr,ednf->erf", low, slope)
        grad_a = grad_a + dot("ednr,ednw->erw", back, rows_x)
        blocks = following

    joined = ADAPTER_SCALE * jnp.concatenate([grad_a, grad_b], axis=2)
    pieces = [joined] + [dp_shift(joined, k) for k in range(1, halves)]
    stacked = jnp.stack(pieces[::-1])
    whole = jnp.roll(stacked, me + 1, axis=0)
    whole_a = whole[:, :, :, :part].transpose(1, 0, 3, 2).reshape(experts_here, width, -1)
    whole_b = whole[:, :, :, part:].transpose(1, 2, 0, 3).reshape(experts_here, -1, hidden)
    return (whole_a, whole_b)


MESH = pl.DeviceIdType.MESH
LANES = 256


def chunks(extent, size, body):
    def step(n, carry):
        body(pl.ds(pl.multiple_of(n * size, size), size))
        return carry

    lax.fori_loop(0, extent // size, step, 0)


def whole_kernel(
    ring, inner, capacity,
    tok, grd, route, wgt, first, second,
    out_a, out_b,
    blk_c, blk_x, blk_g, edge_g, stg_x, stg_g, row_x, row_g, w_buf, srt, pre, slope, lowb,
    snd_p, rcv_p, snd_l, rcv_l, snd_b, rcv_b, acc_a, acc_b, got_a, got_b, end_a, end_b, raw_g, its_g,
    loc_sem, dps_sem, dpr_sem, zs_sem, zr_sem, gs_sem, gr_sem, ps_sem, pr_sem, qs_sem, qr_sem, bs_sem, br_sem,
    fs_sem, fr_sem,
):
    column, me = lax.axis_index("expert"), lax.axis_index("dp")
    z, p0 = column // inner, column % inner
    other = 1 - me
    experts_here, part, hidden = w_buf.shape
    half = hidden // 2
    tok_rows = tok.shape[0]
    group = experts_here * capacity
    total_rows = inner * group
    each = inner * capacity
    experts = experts_here * inner * ring
    last = ring - 1
    inside = (z > 0) & (z < last)

    def unit(k):
        near = jnp.where(inside, jnp.where(k == 1, 2, jnp.where(k == 2, 0, k)), k)
        flipped = jnp.where(z < ring // 2, near, last - near)
        return jnp.where(k == 0, z, flipped)

    barrier = pltpu.get_barrier_semaphore()

    def greet(device):
        pl.semaphore_signal(barrier, inc=1, device_id=device, device_id_type=MESH)

    for p in range(1, inner):
        greet((z * inner + (p0 + p) % inner, me))
    greet((column, other))

    @pl.when(z > 0)
    def _():
        greet((column - inner, me))

    @pl.when(z < last)
    def _():
        greet((column + inner, me))

    pl.semaphore_wait(
        barrier, inner + jnp.where(z > 0, 1, 0) + jnp.where(z < last, 1, 0)
    )

    my_cols = pl.ds(pl.multiple_of(me * part, part), part)
    its_cols = pl.ds(pl.multiple_of(other * part, part), part)
    my_hid = pl.ds(pl.multiple_of(me * half, half), half)
    its_hid = pl.ds(pl.multiple_of(other * half, half), half)
    blocks = (blk_c, blk_x, blk_g)
    core = p0 % 2
    far_first = (2, 3 - 2 * core, 1 + 2 * core)
    ordered = tuple(zip((*far_first, 0), (0, 1, 2, 2)))

    def remote(src, dst, send, recv, device):
        return pltpu.make_async_remote_copy(
            src_ref=src, dst_ref=dst, send_sem=send, recv_sem=recv,
            device_id=device, device_id_type=MESH,
        )

    def arrived(ref, sem):
        remote(ref, ref, fs_sem.at[0], sem, (column, other)).wait_recv()

    def sent(ref, sem):
        remote(ref, ref, sem, fr_sem.at[0], (column, other)).wait_send()

    local_x = pltpu.make_async_copy(tok.at[:, my_cols], blk_x.at[z, 0], loc_sem.at[0])
    local_g = pltpu.make_async_copy(grd, raw_g, loc_sem.at[1])
    local_w = pltpu.make_async_copy(wgt, w_buf, loc_sem.at[2])

    def dp_copy(item):
        src = (blk_c.at[z, 0], tok.at[:, its_cols], its_g)[item]
        return remote(
            src, blocks[item].at[z, 1], dps_sem.at[item], dpr_sem.at[item], (column, other)
        )

    def z_copy(way, u, s, item, src=None):
        step = inner if way == 0 else -inner
        dst = blocks[item].at[u, s]
        return remote(
            dst if src is None else src, dst,
            zs_sem.at[way, item], zr_sem.at[u, s, item], (column + step, me),
        )

    def rows_of(p):
        return pl.ds(pl.multiple_of((p0 + p) % inner * group, group), group)

    def z_piece(way, u, s, p, turn):
        step = inner if way == 0 else -inner
        return remote(
            edge_g.at[u, s, rows_of(p), :], stg_g.at[u, s, rows_of(p), :],
            gs_sem.at[0], gr_sem.at[u, s, turn], (column + step, me),
        )

    def to_end(way):
        return (z == last - 1) if way == 0 else (z == 1)

    def z_send(u, s, item, up, down, src=None):
        for way, on in ((0, up & (z < last)), (1, down & (z > 0))):
            if item < 2:
                @pl.when(on)
                def _():
                    z_copy(way, u, s, item, src).start()
            else:
                @pl.when(on & jnp.logical_not(to_end(way)))
                def _():
                    z_copy(way, u, s, item, src).start()

                @pl.when(on & to_end(way))
                def _():
                    fill(1, edge_g, u, s, last if way == 0 else 0)
                    for p, turn in ordered:
                        z_piece(way, u, s, p, turn).start()

    def relay(u, s, item):
        z_copy(0, u, s, item).wait_recv()
        z_send(u, s, item, u < z, u > z)

    yes = z >= 0
    local_g.start()
    dp_copy(1).start()
    z_send(z, 0, 1, yes, yes, tok.at[:, my_cols])
    local_x.start()

    labels = lax.broadcasted_iota(jnp.int32, (experts, tok_rows), 0)
    ones = [jnp.where(route[k : k + 1, :] == labels, 1.0, 0.0) for k in range(2)]
    earlier = jnp.where(
        lax.broadcasted_iota(jnp.int32, (tok_rows, tok_rows), 0)
        < lax.broadcasted_iota(jnp.int32, (tok_rows, tok_rows), 1),
        1.0,
        0.0,
    ).astype(jnp.bfloat16)
    before = [
        jnp.dot(one.astype(jnp.bfloat16), earlier, preferred_element_type=F32) for one in ones
    ]
    before[1] = before[1] + jnp.sum(ones[0], axis=1, keepdims=True)
    base = lax.broadcasted_iota(jnp.int32, (experts, tok_rows), 0).astype(F32) * capacity
    for k in range(2):
        code = jnp.sum(ones[k] * (before[k] + base), axis=0, keepdims=True)
        blk_c[z, 0, k : k + 1, :] = code.astype(jnp.int32)
    dp_copy(0).start()
    local_g.wait()
    for cols, put in ((my_hid, blk_g.at[z, 0]), (its_hid, its_g)):
        for k in range(2):
            put[k] = raw_g[:, k, cols]
    dp_copy(2).start()
    z_send(z, 0, 0, yes, yes)
    local_w.start()

    def plane_copy(kind, u, s, p):
        stage, rows = ((stg_x, row_x), (stg_g, row_g))[kind]
        peer = (p0 + p) % inner
        return remote(
            stage.at[u, s, pl.ds(pl.multiple_of(peer * group, group), group), :],
            rows.at[u, s, pl.ds(pl.multiple_of(p0 * group, group), group), :],
            ps_sem.at[kind], pr_sem.at[kind, u, s], (z * inner + peer, me),
        )

    def plane_wait(kind, u, s):
        rows = (row_x, row_g)[kind]
        arrived(rows.at[u, s, pl.ds(0, (inner - 1) * group), :], pr_sem.at[kind, u, s])

    def fill(kind, stage, u, s, plane):
        place = plane * total_rows + lax.broadcasted_iota(
            jnp.int32, (total_rows, tok_rows), 0
        )
        picks = [blk_c[u, s, k : k + 1, :] == place for k in range(2)]
        if kind == 0:
            chosen = jnp.where(picks[0] | picks[1], 1.0, 0.0).astype(jnp.bfloat16)
        else:
            chosen = jnp.concatenate(
                [jnp.where(pick, 1.0, 0.0).astype(jnp.bfloat16) for pick in picks], axis=1
            )

        def one(cols):
            if kind == 0:
                block = blk_x[u, s, :, cols]
            else:
                block = blk_g[u, s, :, :, cols].reshape(2 * tok_rows, LANES)
            stage[u, s, :, cols] = jnp.dot(
                chosen, block, preferred_element_type=F32
            ).astype(jnp.bfloat16)

        chunks(stage.shape[-1], LANES, one)

    def pack(kind, u, s):
        stage, rows = ((stg_x, row_x), (stg_g, row_g))[kind]
        fill(kind, stage, u, s, z)
        for p in far_first:
            plane_copy(kind, u, s, p).start()
        rows[u, s, rows_of(0), :] = stage[u, s, rows_of(0), :]

    def pass_far(u, s, turn):
        arrived(stg_g.at[u, s, rows_of(0), :], gr_sem.at[u, s, turn])
        plane_copy(1, u, s, far_first[turn]).start()

    def pass_rest(u, s):
        arrived(stg_g.at[u, s, pl.ds(0, 2 * group), :], gr_sem.at[u, s, 2])
        plane_copy(1, u, s, far_first[2]).start()
        row_g[u, s, rows_of(0), :] = stg_g[u, s, rows_of(0), :]

    def pass_on(u, s):
        pass_far(u, s, 0)
        pass_far(u, s, 1)
        pass_rest(u, s)

    def partner_copy(u, s, item):
        src, dst = ((snd_p, rcv_p), (snd_l, rcv_l))[item]
        return remote(
            src.at[u, s], dst.at[u, 1 - s], qs_sem.at[item], qr_sem.at[u, 1 - s, item],
            (column, other),
        )

    def partner_wait(u, s, item):
        src, dst = ((snd_p, rcv_p), (snd_l, rcv_l))[item]
        remote(
            src.at[u, s], dst.at[u, s], qs_sem.at[item], qr_sem.at[u, s, item],
            (column, other),
        ).wait_recv()

    def matmul(u, s, par):
        plane_wait(0, u, s)

        def sort(cols):
            wide = row_x[u, s, :, cols].astype(F32).reshape(inner, experts_here, capacity, LANES)
            for e in range(experts_here):
                srt[par, s, e, :, cols] = wide[:, e].reshape(each, LANES).astype(jnp.bfloat16)

        chunks(part, LANES, sort)

        def product(e, cols):
            return jnp.dot(srt[par, s, e], w_buf[e, :, cols], preferred_element_type=F32)

        for e in range(experts_here):
            snd_p[u, s, e] = product(e, its_hid).astype(jnp.bfloat16)
            snd_l[u, s, e, :, :each] = lax.dot_general(
                first[e, :, my_cols], srt[par, s, e], (((1,), (1,)), ((), ())),
                preferred_element_type=F32,
            )
        partner_copy(u, s, 0).start()
        partner_copy(u, s, 1).start()
        for e in range(experts_here):
            pre[par, s, e] = product(e, my_hid)

    def back_copy(u, s):
        return remote(
            snd_b.at[u, s], rcv_b.at[u, 1 - s], bs_sem.at[0], br_sem.at[u, 1 - s],
            (column, other),
        )

    def back_wait(u, s):
        remote(
            snd_b.at[u, s], rcv_b.at[u, s], bs_sem.at[0], br_sem.at[u, s], (column, other)
        ).wait_recv()

    def act(u, par, which=(0, 1)):
        for s in which:
            partner_wait(u, s, 0)
            partner_wait(u, s, 1)
            for e in range(experts_here):
                low = (snd_l[u, s, e, :, :each] + rcv_l[u, s, e, :, :each]).astype(jnp.bfloat16)
                lowb[par, s, e, :, :each] = low

                def one(n, carry):
                    at = pl.multiple_of(n * LANES, LANES)
                    cols = pl.ds(at, LANES)
                    adapt = lax.dot_general(
                        lowb[par, s, e, :, :each],
                        second[e, :, pl.ds(pl.multiple_of(me * half + at, LANES), LANES)],
                        (((0,), (0,)), ((), ())),
                        preferred_element_type=F32,
                    )
                    value = (
                        pre[par, s, e, :, cols]
                        + rcv_p[u, s, e, :, cols].astype(F32)
                        + ADAPTER_SCALE * adapt
                    )
                    pre[par, s, e, :, cols] = silu_slope(value)
                    return carry

                lax.fori_loop(0, half // LANES, one, 0)

    def slopes(u, par):
        for s in range(2):
            plane_wait(1, u, s)

            def one(n, carry):
                cols = pl.ds(pl.multiple_of(n * LANES, LANES), LANES)
                wide = row_g[u, s, :, cols].astype(F32)
                wide = wide.reshape(inner, experts_here, capacity, LANES)
                for e in range(experts_here):
                    given = wide[:, e].reshape(each, LANES)
                    slope[s, e, :, cols] = (given * pre[par, s, e, :, cols]).astype(jnp.bfloat16)
                return carry

            lax.fori_loop(0, half // LANES, one, 0)
            for e in range(experts_here):
                snd_b[u, s, e, :, :each] = lax.dot_general(
                    second[e, :, my_hid], slope[s, e], (((1,), (1,)), ((), ())),
                    preferred_element_type=F32,
                )
            back_copy(u, s).start()

    def gradients(u, par, late, final):
        for s in range(2):
            for e in range(experts_here):
                acc_b[late, e] += jnp.dot(
                    lowb[par, s, e, :, :each], slope[s, e], preferred_element_type=F32
                )

        @pl.when(final)
        def _():
            end_b[0] = acc_b[1].astype(jnp.bfloat16)
            ends[1].start()

        for s in range(2):
            back_wait(u, s)
            for e in range(experts_here):
                back = (snd_b[u, s, e, :, :each] + rcv_b[u, s, e, :, :each]).astype(jnp.bfloat16)
                acc_a[late, e] += jnp.dot(back, srt[par, s, e], preferred_element_type=F32)

        @pl.when(final)
        def _():
            end_a[0] = acc_a[1].astype(jnp.bfloat16)
            ends[0].start()

    ends = [
        remote(ref.at[0], ref.at[1], fs_sem.at[2 + i], fr_sem.at[2 + i], (column, other))
        for i, ref in enumerate((end_a, end_b))
    ]
    firsts = [
        remote(src.at[0], dst, fs_sem.at[i], fr_sem.at[i], (column, other))
        for i, (src, dst) in enumerate(((acc_a, got_a), (acc_b, got_b)))
    ]
    acc_a[...] = jnp.zeros_like(acc_a)
    acc_b[...] = jnp.zeros_like(acc_b)

    def relay_x(u, s):
        for item in (0, 1):
            relay(u, s, item)

    def twice(step):
        def run(s, carry):
            step(s)
            return carry

        lax.fori_loop(0, 2, run, 0)

    z_send(z, 0, 2, yes, yes)
    local_x.wait()
    pack(0, z, 0)
    for item in (0, 1):
        dp_copy(item).wait_recv()
        z_send(z, 1, item, yes, yes)
    pack(0, z, 1)
    local_w.wait()
    at_end = jnp.logical_not(inside)

    def when(condition, step, *args):
        @pl.when(condition)
        def _():
            step(*args)

    def bring_x(k, s):
        relay_x(unit(k), s)
        pack(0, unit(k), s)

    def first_x(s):
        relay_x(unit(1), s)
        when(inside, relay_x, unit(2), s)
        pack(0, unit(1), s)

    def near_g():
        relay_x(unit(3), 1)
        near = unit(1)
        twice(lambda i: z_send(near, i, 2, near < z, near > z))

    def bring_g(k, s):
        relay(unit(k), s, 2)
        pack(1, unit(k), s)

    def second_g(s):
        z_copy(0, unit(1), s, 2).wait_recv()
        relay(unit(2), s, 2)
        pack(1, unit(1), s)

    def own_g(s):
        @pl.when(s == 1)
        def _():
            dp_copy(2).wait_recv()
            z_send(z, 1, 2, yes, yes)

        pack(1, z, s)

    def finish(kk, inner_carry):
        when((kk == 2) & at_end, pass_on, unit(3), 0)
        when(inside | (kk < 2), act, unit(kk), kk % 2)
        slopes(unit(kk), kk % 2)

        @pl.when((kk == 2) & at_end)
        def _():
            pass_far(unit(3), 1, 0)
            act(unit(3), 1, (0,))
            pass_far(unit(3), 1, 1)
            act(unit(3), 1, (1,))
            pass_rest(unit(3), 1)

        gradients(unit(kk), kk % 2, jnp.where(kk >= 2, 1, 0), kk == 3)

        @pl.when(kk == 1)
        def _():
            for end in firsts:
                end.start()

        return inner_carry

    def body(b, carry):
        k, s = b // 2, b % 2
        when((b == 1) | (b == 2), first_x, b - 1)
        when((b == 4) & at_end, bring_x, 2, 1)
        when(((b == 5) | (b == 6)) & at_end, bring_x, 3, b - 5)
        when((b == 7) & at_end, pass_on, unit(2), 0)
        when((b == 7) & at_end, act, unit(2), 0)
        when(((b == 3) | (b == 4)) & inside, pack, 0, unit(2), b - 3)
        when((b == 4) & inside, relay_x, unit(3), 0)
        when(((b == 5) | (b == 6)) & inside, pack, 0, unit(3), b - 5)
        matmul(unit(k), s, k % 2)
        when(k == 0, own_g, s)
        when((k == 1) & at_end, pass_on, unit(1), s)
        when((b == 3) & at_end, bring_x, 2, 0)
        when((k == 1) & inside, second_g, s)
        when((b == 4) & inside, near_g)
        when((k == 2) & inside, pack, 1, unit(2), s)
        when((k == 3) & inside, bring_g, 3, s)
        when((b == 7) & at_end, pass_on, unit(2), 1)
        begin = jnp.where(
            b == 2,
            0,
            jnp.where(
                b == jnp.where(inside, 4, 3),
                1,
                jnp.where(b == jnp.where(inside, 6, 7), 2, jnp.where(b == 7, 3, 4)),
            ),
        )
        stop = jnp.where(begin == 4, 4, jnp.where(b == 7, 4, begin + 1))
        lax.fori_loop(begin, stop, finish, 0)
        return carry

    lax.fori_loop(0, 2 * ring, body, 0)
    out_a[:, :, my_cols] = acc_a[0] + end_a[0].astype(F32)
    out_b[:, :, my_hid] = acc_b[0] + end_b[0].astype(F32)

    for item, ref in enumerate(blocks):
        for n in range(1, ring):
            up, down = z == n - 1, z == ring - n
            if item == 2:
                up, down = up & (z < last - 1), down & (z > 1)
            when(up, sent, ref.at[pl.ds(0, n)], zs_sem.at[0, item])
            when(down, sent, ref.at[pl.ds(0, n)], zs_sem.at[1, item])
    when(inside, sent, edge_g.at[pl.ds(0, last)], gs_sem.at[0])
    share = ring * (inner - 1) // inner
    sent(stg_x.at[pl.ds(0, share)], ps_sem.at[0])
    sent(stg_g.at[pl.ds(0, share)], ps_sem.at[1])
    sent(snd_p, qs_sem.at[0])
    sent(snd_l, qs_sem.at[1])
    sent(snd_b, bs_sem.at[0])
    for item in range(3):
        dp_copy(item).wait_send()
    for end in firsts:
        end.wait()
    for end in ends:
        end.wait()
    out_a[:, :, its_cols] = got_a[...] + end_a[1].astype(F32)
    out_b[:, :, its_hid] = got_b[...] + end_b[1].astype(F32)


def scale_kernel(in_a, in_b, out_a, out_b):
    out_a[...] = ADAPTER_SCALE * in_a[...]
    out_b[...] = ADAPTER_SCALE * in_b[...]


def whole(tokens, route, gate_output_gradient, frozen_gate_weight, adapter_first, adapter_second):
    experts_here, part, hidden = frozen_gate_weight.shape
    columns = lax.axis_size("expert")
    tok_rows, width = tokens.shape
    rank = adapter_second.shape[1]
    ring, inner = RING, columns // RING
    capacity = 3 * tok_rows * route.shape[1] // (experts_here * columns)
    half, each, rows = hidden // 2, inner * capacity, inner * experts_here * capacity
    bf16 = jnp.bfloat16
    dma = pltpu.SemaphoreType.DMA
    vmem = pl.BlockSpec(memory_space=pltpu.VMEM)
    hbm = pl.BlockSpec(memory_space=pl.ANY)
    lanes = -(-each // 128) * 128
    out_a, out_b = pl.pallas_call(
        functools.partial(whole_kernel, ring, inner, capacity),
        out_shape=(
            jax.ShapeDtypeStruct((experts_here, rank, width), F32),
            jax.ShapeDtypeStruct((experts_here, rank, hidden), F32),
        ),
        in_specs=[hbm, hbm, vmem, hbm, vmem, vmem],
        out_specs=(vmem, vmem),
        scratch_shapes=[
            pltpu.VMEM((ring, 2, 2, tok_rows), jnp.int32),
            pltpu.VMEM((ring, 2, tok_rows, part), bf16),
            pltpu.VMEM((ring, 2, 2, tok_rows, half), bf16),
            pltpu.VMEM((ring, 2, rows, half), bf16),
            pltpu.VMEM((ring, 2, rows, part), bf16),
            pltpu.VMEM((ring, 2, rows, half), bf16),
            pltpu.VMEM((ring, 2, rows, part), bf16),
            pltpu.VMEM((ring, 2, rows, half), bf16),
            pltpu.VMEM((experts_here, part, hidden), bf16),
            pltpu.VMEM((2, 2, experts_here, each, part), bf16),
            pltpu.VMEM((2, 2, experts_here, each, half), F32),
            pltpu.VMEM((2, experts_here, each, half), bf16),
            pltpu.VMEM((2, 2, experts_here, rank, lanes), bf16),
            pltpu.VMEM((ring, 2, experts_here, each, half), bf16),
            pltpu.VMEM((ring, 2, experts_here, each, half), bf16),
            pltpu.VMEM((ring, 2, experts_here, rank, lanes), F32),
            pltpu.VMEM((ring, 2, experts_here, rank, lanes), F32),
            pltpu.VMEM((ring, 2, experts_here, rank, lanes), F32),
            pltpu.VMEM((ring, 2, experts_here, rank, lanes), F32),
            pltpu.VMEM((2, experts_here, rank, part), F32),
            pltpu.VMEM((2, experts_here, rank, half), F32),
            pltpu.VMEM((experts_here, rank, part), F32),
            pltpu.VMEM((experts_here, rank, half), F32),
            pltpu.VMEM((2, experts_here, rank, part), bf16),
            pltpu.VMEM((2, experts_here, rank, half), bf16),
            pltpu.VMEM((tok_rows, 2, hidden), bf16),
            pltpu.VMEM((2, tok_rows, half), bf16),
            dma((3,)),
            dma((3,)),
            dma((3,)),
            dma((2, 3)),
            dma((ring, 2, 3)),
            dma((1,)),
            dma((ring, 2, 3)),
            dma((2,)),
            dma((2, ring, 2)),
            dma((2,)),
            dma((ring, 2, 2)),
            dma((1,)),
            dma((ring, 2)),
            dma((4,)),
            dma((4,)),
        ],
        compiler_params=pltpu.CompilerParams(
            collective_id=0, has_side_effects=True, vmem_limit_bytes=58 * 1024 * 1024
        ),
        name="whole",
    )(
        tokens,
        gate_output_gradient,
        route.T,
        frozen_gate_weight,
        adapter_first.transpose(0, 2, 1),
        adapter_second,
    )
    scaled_a, scaled_b = pl.pallas_call(
        scale_kernel,
        out_shape=(
            jax.ShapeDtypeStruct(out_a.shape, F32),
            jax.ShapeDtypeStruct(out_b.shape, F32),
        ),
        in_specs=[vmem, vmem],
        out_specs=(vmem, vmem),
        name="scale",
    )(out_a, out_b)
    return (scaled_a.transpose(0, 2, 1), scaled_b)


def solution(mesh):
    columns, halves = mesh.shape["expert"], mesh.shape["dp"]
    fits = halves == 2 and columns % RING == 0 and columns // RING == 4
    return jax.shard_map(
        whole if fits else local,
        mesh=mesh,
        in_specs=(
            P(("expert", "dp"), None),
            P(("expert", "dp"), None),
            P(("expert", "dp"), None, None),
            P("expert", "dp", None),
            P("expert", None, None),
            P("expert", None, None),
        ),
        out_specs=(P("expert", None, None), P("expert", None, None)),
        check_vma=False,
    )
```
